32 devices in a mesh: seq: 16 (over z, y, x), head: 2 (over core).
Axes of the slice: x: 2, y: 2, z: 4, core: 2. Of those that a mesh axis runs over, the one named last changes fastest.
Arguments:
- tokens: bfloat16 [8192, 3584], P('seq', 'head'), may hold values from -6 to 6
- pre_gain: float32 [3584], replicated, may hold values from 0.5 to 1.5
- query_weight: bfloat16 [3584, 2048], P(None, 'head'), may hold values from -0.375 to 0.375
- key_weight: bfloat16 [3584, 1024], P(None, 'head'), may hold values from -0.375 to 0.375
- value_weight: bfloat16 [3584, 1024], P(None, 'head'), may hold values from -0.09375 to 0.09375
- out_weight: bfloat16 [2048, 3584], P('head'), may hold values from -0.5 to 0.5
- post_gain: float32 [3584], P('head'), may hold values from 0.5 to 1.5
Outputs:
- layer_out: bfloat16 [8192, 3584], P('seq', 'head')
The draws below stay inside these ranges and needn't reach their ends.
All inputs are finite; a program needn't handle non-finite values.
Results may differ from the reference program's by a relative error of at most 0.013.
The reference program's roundings to bfloat16 on the way count: a program that leaves them out, or rounds other values in their place, can miss the bound.
Values may be sent and summed in bfloat16 or wider, within the bound.
No kernel may reach another device: no remote copies, remote signals or barrier semaphores. Data moves between devices by JAX's collectives and lax.ppermute only.
A program may use at most 192 MiB of HBM per device.

```python
import jax
import jax.numpy as jnp
from jax import lax

D = 3584
QH = 8
KVH = 4
HD = 256
WINDOW = 4096
TOK_DEV = 512
TOKENS = 8192


def draw_out_weight(key, part):
    key_entries = jax.random.fold_in(key, 11)
    key_columns = jax.random.fold_in(key, 12)
    fan_in = QH * HD
    ramp = 3.0 ** (jnp.arange(D, dtype=jnp.float32) / D)
    column_scale = jnp.exp(jax.random.uniform(key_columns, (D,), jnp.float32) * jnp.log(10.0)) * ramp / 6.0
    entries = jax.random.truncated_normal(key_entries, -4.0, 4.0, (fan_in, D), jnp.float32)
    matrix = entries * column_scale[None, :] * (fan_in * 1.0) ** (-0.5)
    return jnp.clip(matrix, -0.5, 0.5).astype(jnp.bfloat16)


def block_scale(stream_key, shape, split, smallest, high):
    level = 1.0
    for dim, shards_of in split:
        steps = jax.random.uniform(jax.random.fold_in(jax.random.fold_in(stream_key, 6), dim), (shards_of,), jnp.float32, smallest / len(split), high / len(split))
        level = level * jnp.repeat(jnp.exp(steps), shape[dim] // shards_of).reshape((-1,) + (1,) * (len(shape) - 1 - dim))
    return level


def scatter_about(rng, shape, width, limit, pieces=(), held_as=jnp.bfloat16):
    drawn = width * jax.random.normal(rng, shape, jnp.float32)
    if pieces:
        drawn = drawn * block_scale(rng, shape, pieces, -0.22, 0.18)
    return jnp.clip(drawn, -limit, limit).astype(held_as)


def setup_inputs(seed: int = 0) -> dict:
    streams_of = jax.random.split(jax.random.key(seed), 8)
    return {
        "tokens": scatter_about(streams_of[0], (TOKENS, D), 1.0, 6.0, ((0, 16), (1, 2))),
        "pre_gain": jnp.clip(1.0 + 0.1 * jax.random.normal(streams_of[1], (D,), jnp.float32), 0.5, 1.5),
        "query_weight": scatter_about(streams_of[2], (D, QH * HD), (D // 16) ** -0.5, 0.375, ((1, 2),)),
        "key_weight": scatter_about(streams_of[3], (D, KVH * HD), (D // 16) ** -0.5, 0.375, ((1, 2),)),
        "value_weight": scatter_about(streams_of[4], (D, KVH * HD), D ** -0.5, 0.09375, ((1, 2),)),
        "out_weight": draw_out_weight(jax.random.fold_in(streams_of[7], 71), 0),
        "post_gain": jnp.clip(1.0 + 0.1 * jax.random.normal(streams_of[6], (D,), jnp.float32), 0.5, 1.5),
    }


softcap_limit = 50.0
rope_base = 10000.0
norm_epsilon = 1e-06

def rms_scale(values):
    return lax.rsqrt(lax.optimization_barrier(jnp.sum(values * values, axis=-1, keepdims=True)) / values.shape[-1] + norm_epsilon)

def rotate(values, positions):
    midpoint = values.shape[-1] // 2
    frequency = jnp.exp(-jnp.log(rope_base) * (2.0 * jnp.arange(midpoint, dtype=jnp.float32) / values.shape[-1]))
    angles = positions.astype(jnp.float32)[:, None] * frequency[None, :]
    cosine = jnp.cos(angles)[:, None, :]
    sine_part = jnp.sin(angles)[:, None, :]
    leading = values[..., :midpoint]
    trailing = values[..., midpoint:]
    return jnp.concatenate([leading * cosine - trailing * sine_part, trailing * cosine + leading * sine_part], axis=-1)

def reference(tokens, pre_gain, query_weight, key_weight, value_weight, out_weight, post_gain):
    widened = tokens.astype(jnp.float32)
    normed = (widened * rms_scale(widened) * pre_gain).astype(jnp.bfloat16)
    positions = jnp.arange(TOKENS, dtype=jnp.int32)
    queries = rotate(jnp.dot(normed, query_weight, preferred_element_type=jnp.float32).reshape(TOKENS, QH, HD), positions).astype(jnp.bfloat16)
    keys_all = rotate(jnp.dot(normed, key_weight, preferred_element_type=jnp.float32).reshape(TOKENS, KVH, HD), positions).astype(jnp.bfloat16)
    values_all = jnp.dot(normed, value_weight, preferred_element_type=jnp.float32).reshape(TOKENS, KVH, HD).astype(jnp.bfloat16)
    queries = lax.optimization_barrier(queries).astype(jnp.float32)
    keys_all = lax.optimization_barrier(keys_all).astype(jnp.float32)
    values_all = lax.optimization_barrier(values_all).astype(jnp.float32)
    group_size = QH // KVH
    padding = jnp.zeros((WINDOW, KVH, HD), jnp.float32)
    keys_padded = jnp.concatenate([padding, keys_all], axis=0)
    values_padded = jnp.concatenate([padding, values_all], axis=0)

    def one_block(block_index):
        first_row = block_index * TOK_DEV
        query_block = lax.dynamic_slice_in_dim(queries, first_row, TOK_DEV, 0).reshape(TOK_DEV, KVH, group_size, HD)
        key_block = lax.dynamic_slice_in_dim(keys_padded, first_row, WINDOW + TOK_DEV, 0)
        value_block = lax.dynamic_slice_in_dim(values_padded, first_row, WINDOW + TOK_DEV, 0)
        query_index = first_row + jnp.arange(TOK_DEV, dtype=jnp.int32)
        key_index = first_row - WINDOW + jnp.arange(WINDOW + TOK_DEV, dtype=jnp.int32)
        scores = jnp.einsum('qkgd,skd->kgqs', query_block, key_block) * HD ** (-0.5)
        capped = softcap_limit * jnp.tanh(scores / softcap_limit)
        offset = query_index[:, None] - key_index[None, :]
        allowed = (offset >= 0) & (offset < WINDOW) & (key_index[None, :] >= 0)
        weights = jnp.where(allowed, jnp.exp(capped), 0.0)
        denominator = lax.optimization_barrier(jnp.sum(weights, axis=-1))
        rounded = lax.optimization_barrier(weights.astype(jnp.bfloat16)).astype(jnp.float32)
        numerator = jnp.einsum('kgqs,skd->qkgd', rounded, value_block)
        attended_block = numerator / jnp.transpose(denominator, (2, 0, 1))[..., None]
        return attended_block.astype(jnp.bfloat16).reshape(TOK_DEV, QH * HD)
    attended = lax.map(one_block, jnp.arange(TOKENS // TOK_DEV, dtype=jnp.int32)).reshape(TOKENS, QH * HD)
    branch = jnp.dot(attended, out_weight, preferred_element_type=jnp.float32)
    return (widened + post_gain * branch * rms_scale(branch)).astype(jnp.bfloat16)
```

```python
import functools

import jax
import jax.numpy as jnp
from jax import lax
from jax.experimental import pallas as pl
from jax.experimental.pallas import tpu as pltpu
from jax.sharding import PartitionSpec as P

HD = 256
WINDOW = 4096

softcap_limit = 50.0
rope_base = 10000.0
norm_epsilon = 1e-06


LOG2E = 1.4426950408889634
ROW_CHUNK = 256


def rope_tables(positions, head_dim):
    midpoint = head_dim // 2
    frequency = jnp.exp(
        -jnp.log(rope_base) * (2.0 * jnp.arange(midpoint, dtype=jnp.float32) / head_dim)
    )
    angles = positions.astype(jnp.float32)[:, None] * frequency[None, :]
    return jnp.cos(angles)[:, None, :], jnp.sin(angles)[:, None, :]


def rotate(values, tables):
    cosine, sine_part = tables
    midpoint = values.shape[-1] // 2
    leading = values[..., :midpoint]
    trailing = values[..., midpoint:]
    return jnp.concatenate(
        [leading * cosine - trailing * sine_part, trailing * cosine + leading * sine_part], axis=-1
    )


def attend_kernel(n_q, n_kv, window_blocks, first, last, *refs):
    scalars = refs[0]
    refs = refs[1:]
    q_refs, refs = refs[:n_q], refs[n_q:]
    kv_refs, refs = refs[:n_kv], refs[n_kv:]
    if not first:
        acc_in, den_in, refs = refs[0], refs[1], refs[2:]
    if last:
        o_refs, refs = refs[:n_q], refs[n_q:]
        q_all, kv_all, acc, den = refs
    else:
        acc, den, refs = refs[0], refs[1], refs[2:]
        q_all, kv_all = refs
    rows = q_refs[0].shape[0]
    heads = q_refs[0].shape[1] // HD
    lanes = den.shape[-1] // heads
    for r in range(n_q):
        q_all[r] = q_refs[r][...]
    for r in range(n_kv):
        kv_all[r] = kv_refs[r][...]
    if first:
        acc[...] = jnp.zeros_like(acc)
        den[...] = jnp.zeros_like(den)
    elif last:
        acc[...] = acc_in[...]
        den[...] = den_in[...]

    chunk = min(ROW_CHUNK, rows)

    def pair(r, n, delta, masked):
        keys = kv_all[n, :, :HD]
        values = kv_all[n, :, HD:]
        for head in range(heads):
            for start in range(0, rows, chunk):
                at = slice(start, start + chunk)
                columns = slice(head * HD, (head + 1) * HD)
                scores = lax.dot_general(
                    q_all[r, at, columns],
                    keys,
                    (((1,), (1,)), ((), ())),
                    preferred_element_type=jnp.float32,
                )
                weights = jnp.exp2(
                    jnp.tanh(scores * (HD ** (-0.5) / softcap_limit)) * (softcap_limit * LOG2E)
                )
                if masked:
                    offset = (
                        delta * rows
                        + start
                        + lax.broadcasted_iota(jnp.int32, weights.shape, 0)
                        - lax.broadcasted_iota(jnp.int32, weights.shape, 1)
                    )
                    allowed = (offset >= 0) & (offset < window_blocks * rows)
                    weights = jnp.where(allowed, weights, 0.0)
                part = weights[:, :lanes]
                for k in range(lanes, rows, lanes):
                    part = part + weights[:, k : k + lanes]
                lane_at = slice(head * lanes, (head + 1) * lanes)
                den[r, at, lane_at] = den[r, at, lane_at] + part
                acc[r, at, columns] = acc[r, at, columns] + jnp.dot(
                    weights.astype(jnp.bfloat16), values, preferred_element_type=jnp.float32
                )

    def step(t, carry):
        r = t // n_kv
        n = t % n_kv
        key_block = scalars[n_q + n]
        delta = scalars[r] - key_block
        live = key_block >= 0

        @pl.when(live & (delta > 0) & (delta < window_blocks))
        def _():
            pair(r, n, delta, False)

        @pl.when(live & ((delta == 0) | (delta == window_blocks)))
        def _():
            pair(r, n, delta, True)

        return carry

    lax.fori_loop(0, n_q * n_kv, step, 0)
    if last:
        for r in range(n_q):
            for head in range(heads):
                total = jnp.sum(
                    den[r, :, head * lanes : (head + 1) * lanes], axis=-1, keepdims=True
                )
                columns = slice(head * HD, (head + 1) * HD)
                o_refs[r][:, columns] = (acc[r, :, columns] / total).astype(jnp.bfloat16)


def attend(query_blocks, key_blocks, queries, pieces, totals, last):
    n_q, n_kv = len(queries), len(pieces)
    rows, width = queries[0].shape
    heads = width // HD
    lanes = min(128, rows)
    first = totals is None
    acc_shape = jax.ShapeDtypeStruct((n_q, rows, width), jnp.float32)
    den_shape = jax.ShapeDtypeStruct((n_q, rows, heads * lanes), jnp.float32)
    scalars = jnp.stack(list(query_blocks) + list(key_blocks)).astype(jnp.int32)
    vmem = pl.BlockSpec(memory_space=pltpu.VMEM)
    operands = [scalars, *queries, *pieces] + ([] if first else list(totals))
    scratch = [
        pltpu.VMEM((n_q, rows, width), jnp.bfloat16),
        pltpu.VMEM((n_kv, rows, pieces[0].shape[1]), jnp.bfloat16),
    ]
    aliases = {}
    if last:
        out_shape = [jax.ShapeDtypeStruct((rows, width), jnp.bfloat16)] * n_q
        scratch += [
            pltpu.VMEM(acc_shape.shape, jnp.float32),
            pltpu.VMEM(den_shape.shape, jnp.float32),
        ]
    else:
        out_shape = [acc_shape, den_shape]
        if not first:
            aliases = {1 + n_q + n_kv: 0, 2 + n_q + n_kv: 1}
    flops = n_q * n_kv * heads * 4 * rows * rows * HD * 2 // 3
    return pl.pallas_call(
        functools.partial(attend_kernel, n_q, n_kv, WINDOW // rows, first, last),
        out_shape=out_shape,
        in_specs=[pl.BlockSpec(memory_space=pltpu.SMEM)] + [vmem] * (len(operands) - 1),
        out_specs=[vmem] * len(out_shape),
        scratch_shapes=scratch,
        input_output_aliases=aliases,
        compiler_params=pltpu.CompilerParams(vmem_limit_bytes=24 * 1024 * 1024),
        cost_estimate=pl.CostEstimate(
            flops=flops,
            bytes_accessed=n_q * rows * width * 10,
            transcendentals=2 * n_q * n_kv * heads * rows * rows,
        ),
    )(*operands)


def local(tokens, pre_gain, query_weight, key_weight, value_weight, out_weight, post_gain):
    n_seq = lax.axis_size("seq")
    cores = lax.axis_size("head")
    rows, part = tokens.shape
    kv_heads = key_weight.shape[1] // HD
    query_heads = query_weight.shape[1] // HD
    group_size = query_heads // kv_heads
    piece_width = group_size * HD
    plane = cores * kv_heads
    hops = WINDOW // (rows * plane)
    seq = lax.axis_index("seq")
    core = lax.axis_index("head")
    place = seq % plane
    column = place % kv_heads

    def over_cores(value, by=1):
        return lax.ppermute(value, "head", [(c, (c + by) % cores) for c in range(cores)])

    def next_plane(value):
        return lax.ppermute(value, "seq", [(i, i + plane) for i in range(n_seq - plane)])

    def route(turn):
        pairs = []
        for s in range(n_seq):
            base, at = s - s % plane, s % plane
            y, x = at // kv_heads, at % kv_heads
            for c in range(cores):
                target = base + c * kv_heads + (x + turn) % kv_heads
                pairs.append((s * cores + c, target * cores + y))
        return pairs

    def spread(value, turn):
        return lax.ppermute(value, ("seq", "head"), route(turn))

    def gather_back(value, turn):
        return lax.ppermute(value, ("seq", "head"), [(b, a) for a, b in route(turn)])

    shards = [tokens] + [over_cores(tokens, by) for by in range(1, cores)]
    widened = [shard.astype(jnp.float32) for shard in shards]
    squares = sum(jnp.sum(w * w, axis=-1, keepdims=True) for w in widened)
    scale = lax.rsqrt(squares / (part * cores) + norm_epsilon)
    full = jnp.concatenate(shards, axis=1)
    if cores == 2:
        swapped = jnp.concatenate(shards[::-1], axis=1)
        full = jnp.where(core == 0, full, swapped)
    else:
        full = lax.all_gather(tokens, "head", axis=1, tiled=True)
    normed = (full.astype(jnp.float32) * scale * pre_gain).astype(jnp.bfloat16)

    positions = seq * rows + jnp.arange(rows, dtype=jnp.int32)
    tables = rope_tables(positions, HD)

    def project(weight, rotated):
        heads = weight.shape[1] // HD
        product = jnp.dot(normed, weight, preferred_element_type=jnp.float32)
        product = product.reshape(rows, heads, HD)
        if rotated:
            product = rotate(product, tables)
        return product.astype(jnp.bfloat16)

    keys = project(key_weight, True)
    values = project(value_weight, False)
    own_pieces = jnp.concatenate([keys, values], axis=-1)
    queries = project(query_weight, True).reshape(rows, query_heads * HD)

    own, sent = [], []
    for turn in range(kv_heads):
        which = (column + turn) % kv_heads
        piece = lax.dynamic_index_in_dim(own_pieces, which, 1, keepdims=False)
        sent.append(piece)
    travelling = [next_plane(piece) for piece in sent]
    q_pieces = []
    for turn in range(kv_heads):
        which = (column + turn) % kv_heads
        piece = lax.dynamic_slice_in_dim(queries, which * piece_width, piece_width, 1)
        q_pieces.append(spread(piece, turn))
    levels = [[spread(piece, turn) for turn, piece in enumerate(sent)]]
    level = [spread(piece, turn) for turn, piece in enumerate(travelling)]
    levels.append(level)
    for _ in range(1, hops):
        level = [next_plane(piece) for piece in level]
        levels.append(level)

    group_base = seq - place
    block_at = [(column - turn) % kv_heads for turn in range(kv_heads)]
    query_blocks = [group_base + core * kv_heads + block_at[turn] for turn in range(kv_heads)]

    def merged(level, lag, turns):
        pieces, blocks = [], []
        for turn in turns:
            for by in range(cores):
                piece = level[turn] if by == 0 else over_cores(level[turn], by)
                source = (core - by) % cores
                pieces.append(piece)
                blocks.append(group_base - lag * plane + source * kv_heads + block_at[turn])
        return pieces, blocks

    totals = None
    for lag, level in enumerate(levels):
        split = [range(kv_heads)] if lag == 0 else [[turn] for turn in range(kv_heads)]
        for index, turns in enumerate(split):
            pieces, blocks = merged(level, lag, turns)
            last = lag == len(levels) - 1 and index == len(split) - 1
            totals = attend(query_blocks, blocks, q_pieces, pieces, totals, last)
    returned = [gather_back(o, turn) for turn, o in enumerate(totals)]

    def out_part(first_column):
        total = None
        for turn in range(kv_heads):
            which = (column + turn) % kv_heads
            block = lax.dynamic_slice(
                out_weight, (which * piece_width, first_column), (piece_width, part)
            )
            product = jnp.dot(returned[turn], block, preferred_element_type=jnp.float32)
            total = product if total is None else total + product
        return total

    arrived = []
    for by in range(1, cores):
        target = (core + by) % cores
        arrived.append(over_cores(out_part(target * part).astype(jnp.bfloat16), by))
    share = out_part(core * part)
    for piece in arrived:
        share = share + piece.astype(jnp.float32)
    square = jnp.sum(share * share, axis=1)
    total_square = square
    for by in range(1, cores):
        total_square = total_square + over_cores(square, by)
    inverse_rms = lax.rsqrt(total_square / (part * cores) + norm_epsilon)[:, None]
    return (tokens.astype(jnp.float32) + post_gain * share * inverse_rms).astype(jnp.bfloat16)


def solution(mesh):
    placed = (
        P("seq", "head"),
        P(),
        P(None, "head"),
        P(None, "head"),
        P(None, "head"),
        P("head", None),
        P("head"),
    )
    return jax.shard_map(
        local, mesh=mesh, in_specs=placed, out_specs=P("seq", "head"), check_vma=False
    )
```

```python
import functools

import jax
import jax.numpy as jnp
from jax import lax
from jax.experimental import pallas as pl
from jax.experimental.pallas import tpu as pltpu
from jax.sharding import PartitionSpec as P

HD = 256
WINDOW = 4096

softcap_limit = 50.0
rope_base = 10000.0
norm_epsilon = 1e-06


LOG2E = 1.4426950408889634
ROW_CHUNK = 256


def rope_tables(positions, head_dim):
    midpoint = head_dim // 2
    frequency = jnp.exp(
        -jnp.log(rope_base) * (2.0 * jnp.arange(midpoint, dtype=jnp.float32) / head_dim)
    )
    angles = positions.astype(jnp.float32)[:, None] * frequency[None, :]
    return jnp.cos(angles), jnp.sin(angles)


def dot(left, right):
    return jnp.dot(left, right, preferred_element_type=jnp.float32)


def project_kernel(normalise, outputs, scalars, *refs):
    shards = []
    if normalise:
        shards, refs = refs[: normalise + 1], refs[normalise + 1 :]
    else:
        normed, refs = refs[0], refs[1:]
    cosine, sine_part, refs = refs[0], refs[1], refs[2:]
    n_weights = 1 + max(weight for blocks in outputs for weight, _, _ in blocks)
    weights, refs = refs[:n_weights], refs[n_weights:]
    if normalise:
        normed, refs = refs[0], refs[1:]
    out_refs, refs = refs[: len(outputs)], refs[len(outputs) :]
    held, arrived = refs
    copies = []
    count = 0
    for index, blocks in enumerate(outputs):
        at = 0
        for weight, width, _ in blocks:
            start = pl.multiple_of(scalars[count], width)
            copy = pltpu.make_async_copy(
                weights[weight].at[:, pl.ds(start, width)],
                held.at[index, :, pl.ds(at, width)],
                arrived.at[count],
            )
            copy.start()
            copies.append(copy)
            at += width
            count += 1
    rows = out_refs[0].shape[0]
    if normalise:
        gain, shards = shards[-1], shards[:-1]
        part = shards[0].shape[1]
        step = min(64, rows)

        def norm_rows(t, carry):
            at = pl.ds(pl.multiple_of(t * step, step), step)
            squares = 0.0
            for shard in shards:
                value = shard[at, :].astype(jnp.float32)
                squares = squares + jnp.sum(value * value, axis=-1, keepdims=True)
            scale = lax.rsqrt(squares / (part * len(shards)) + norm_epsilon)
            for n, shard in enumerate(shards):
                first = pl.multiple_of(scalars[count + n], part)
                columns = pl.ds(first, part)
                value = shard[at, :].astype(jnp.float32) * scale * gain[:, columns]
                normed[at, columns] = value.astype(jnp.bfloat16)
            return carry

        lax.fori_loop(0, rows // step, norm_rows, 0)
    count = 0
    for index, blocks in enumerate(outputs):
        for _ in blocks:
            copies[count].wait()
            count += 1
        chunk = min(256, rows)
        for first in range(0, rows, chunk):
            at = slice(first, first + chunk)
            product = dot(normed[at, :], held[index])
            column = 0
            for _, width, rotated in blocks:
                for head in range(column, column + width, HD):
                    middle = head + HD // 2
                    leading = product[:, head:middle]
                    trailing = product[:, middle : head + HD]
                    if rotated:
                        cos, sin = cosine[at, :], sine_part[at, :]
                        leading, trailing = (
                            leading * cos - trailing * sin,
                            trailing * cos + leading * sin,
                        )
                    out_refs[index][at, head:middle] = leading.astype(jnp.bfloat16)
                    out_refs[index][at, middle : head + HD] = trailing.astype(jnp.bfloat16)
                column += width


def project(source, tables, weights, outputs, starts):
    normalise = isinstance(source, tuple)
    vmem = pl.BlockSpec(memory_space=pltpu.VMEM)
    anywhere = pl.BlockSpec(memory_space=pl.ANY)
    n_copies = sum(len(blocks) for blocks in outputs)
    if normalise:
        shards, firsts, gain = source
        rows, depth = shards[0].shape[0], gain.shape[0]
        operands = [*shards, gain[None, :]]
        scalars = list(starts) + list(firsts)
    else:
        rows, depth = source.shape
        operands = [source]
        scalars = list(starts)
    widths = [sum(width for _, width, _ in blocks) for blocks in outputs]
    out_shape = [jax.ShapeDtypeStruct((rows, width), jnp.bfloat16) for width in widths]
    if normalise:
        out_shape = [jax.ShapeDtypeStruct((rows, depth), jnp.bfloat16)] + out_shape
    return pl.pallas_call(
        functools.partial(project_kernel, len(shards) if normalise else 0, outputs),
        out_shape=out_shape,
        in_specs=[pl.BlockSpec(memory_space=pltpu.SMEM)]
        + [vmem] * (len(operands) + 2)
        + [anywhere] * len(weights),
        out_specs=[vmem] * len(out_shape),
        scratch_shapes=[
            pltpu.VMEM((len(outputs), depth, max(widths)), jnp.bfloat16),
            pltpu.SemaphoreType.DMA((n_copies,)),
        ],
        compiler_params=pltpu.CompilerParams(vmem_limit_bytes=32 * 1024 * 1024),
        cost_estimate=pl.CostEstimate(
            flops=2 * rows * depth * sum(widths),
            bytes_accessed=2 * depth * (rows + sum(widths)),
            transcendentals=0,
        ),
    )(jnp.stack(scalars).astype(jnp.int32), *operands, *tables, *weights)


def out_kernel(n, first, last, scalars, *refs):
    lefts, refs = refs[:n], refs[n:]
    weights, refs = refs[:n], refs[n:]
    if not first:
        total_in, refs = refs[0], refs[1:]
    total, refs = refs[0], refs[1:]
    if last:
        squares, refs = refs[0], refs[1:]
    held, arrived = refs
    rows, width = lefts[0].shape
    out_width = total.shape[1]
    copies = []
    for k in range(n):
        row = pl.multiple_of(scalars[2 * k], width)
        column = pl.multiple_of(scalars[2 * k + 1], out_width)
        copy = pltpu.make_async_copy(
            weights[k].at[pl.ds(row, width), pl.ds(column, out_width)],
            held.at[pl.ds(k * width, width), :],
            arrived.at[k],
        )
        copy.start()
        copies.append(copy)
    for copy in copies:
        copy.wait()
    chunk = min(256, rows)
    columns = 256 if out_width % 256 == 0 else out_width

    def some_rows(t, carry):
        at = pl.ds(pl.multiple_of(t * chunk, chunk), chunk)
        left = jnp.concatenate([ref[at, :] for ref in lefts], axis=1)
        square = jnp.zeros((chunk, 1), jnp.float32)
        for column in range(0, out_width, columns):
            here = slice(column, column + columns)
            value = dot(left, held[:, here])
            if not first:
                value = value + total_in[at, here]
            total[at, here] = value
            if last:
                square = square + jnp.sum(value * value, axis=-1, keepdims=True)
        if last:
            squares[at, :] = square
        return carry

    lax.fori_loop(0, rows // chunk, some_rows, 0)


def out_project(lefts, weights, starts, total, last):
    n = len(lefts)
    rows, width = lefts[0].shape
    out_width = weights[-1].shape[1]
    vmem = pl.BlockSpec(memory_space=pltpu.VMEM)
    anywhere = pl.BlockSpec(memory_space=pl.ANY)
    out_shape = [jax.ShapeDtypeStruct((rows, out_width), jnp.float32)]
    if last:
        out_shape += [jax.ShapeDtypeStruct((rows, 1), jnp.float32)]
    return pl.pallas_call(
        functools.partial(out_kernel, n, total is None, last),
        out_shape=out_shape,
        in_specs=[pl.BlockSpec(memory_space=pltpu.SMEM)]
        + [vmem] * n
        + [anywhere] * n
        + ([] if total is None else [vmem]),
        out_specs=[vmem] * len(out_shape),
        scratch_shapes=[
            pltpu.VMEM((n * width, out_width), jnp.bfloat16),
            pltpu.SemaphoreType.DMA((n,)),
        ],
        input_output_aliases={} if total is None else {1 + 2 * n: 0},
        compiler_params=pltpu.CompilerParams(vmem_limit_bytes=24 * 1024 * 1024),
        cost_estimate=pl.CostEstimate(
            flops=2 * rows * width * n * out_width,
            bytes_accessed=2 * width * n * out_width + 8 * rows * out_width,
            transcendentals=0,
        ),
    )(
        jnp.stack(starts).astype(jnp.int32),
        *lefts,
        *weights,
        *([] if total is None else [total]),
    )


def attend_kernel(n_q, n_kv, window_blocks, first, last, *refs):
    scalars = refs[0]
    refs = refs[1:]
    q_refs, refs = refs[:n_q], refs[n_q:]
    kv_refs, refs = refs[:n_kv], refs[n_kv:]
    if not first:
        acc_in, den_in, refs = refs[0], refs[1], refs[2:]
    if last:
        o_refs, refs = refs[:n_q], refs[n_q:]
        q_all, kv_all, acc, den = refs
    else:
        acc, den, refs = refs[0], refs[1], refs[2:]
        q_all, kv_all = refs
    rows = q_refs[0].shape[0]
    heads = q_refs[0].shape[1] // HD
    lanes = den.shape[-1] // heads
    for r in range(n_q):
        q_all[r] = q_refs[r][...]
    for r in range(n_kv):
        kv_all[r] = kv_refs[r][...]
    if first:
        acc[...] = jnp.zeros_like(acc)
        den[...] = jnp.zeros_like(den)
    elif last:
        acc[...] = acc_in[...]
        den[...] = den_in[...]

    chunk = min(ROW_CHUNK, rows)

    def pair(r, n, delta, masked):
        keys = kv_all[n, :, :HD]
        values = kv_all[n, :, HD:]
        for head in range(heads):
            for start in range(0, rows, chunk):
                at = slice(start, start + chunk)
                columns = slice(head * HD, (head + 1) * HD)
                scores = lax.dot_general(
                    q_all[r, at, columns],
                    keys,
                    (((1,), (1,)), ((), ())),
                    preferred_element_type=jnp.float32,
                )
                weights = jnp.exp2(
                    jnp.tanh(scores * (HD ** (-0.5) / softcap_limit)) * (softcap_limit * LOG2E)
                )
                if masked:
                    offset = (
                        delta * rows
                        + start
                        + lax.broadcasted_iota(jnp.int32, weights.shape, 0)
                        - lax.broadcasted_iota(jnp.int32, weights.shape, 1)
                    )
                    allowed = (offset >= 0) & (offset < window_blocks * rows)
                    weights = jnp.where(allowed, weights, 0.0)
                part = weights[:, :lanes]
                for k in range(lanes, rows, lanes):
                    part = part + weights[:, k : k + lanes]
                lane_at = slice(head * lanes, (head + 1) * lanes)
                den[r, at, lane_at] = den[r, at, lane_at] + part
                acc[r, at, columns] = acc[r, at, columns] + jnp.dot(
                    weights.astype(jnp.bfloat16), values, preferred_element_type=jnp.float32
                )

    def step(t, carry):
        r = t // n_kv
        n = t % n_kv
        key_block = scalars[n_q + n]
        delta = scalars[r] - key_block
        live = key_block >= 0

        @pl.when(live & (delta > 0) & (delta < window_blocks))
        def _():
            pair(r, n, delta, False)

        @pl.when(live & ((delta == 0) | (delta == window_blocks)))
        def _():
            pair(r, n, delta, True)

        return carry

    lax.fori_loop(0, n_q * n_kv, step, 0)
    if last:
        for r in range(n_q):
            for head in range(heads):
                total = jnp.sum(
                    den[r, :, head * lanes : (head + 1) * lanes], axis=-1, keepdims=True
                )
                columns = slice(head * HD, (head + 1) * HD)
                o_refs[r][:, columns] = (acc[r, :, columns] / total).astype(jnp.bfloat16)


def attend(query_blocks, key_blocks, queries, pieces, totals, last):
    n_q, n_kv = len(queries), len(pieces)
    rows, width = queries[0].shape
    heads = width // HD
    lanes = min(128, rows)
    first = totals is None
    acc_shape = jax.ShapeDtypeStruct((n_q, rows, width), jnp.float32)
    den_shape = jax.ShapeDtypeStruct((n_q, rows, heads * lanes), jnp.float32)
    scalars = jnp.stack(list(query_blocks) + list(key_blocks)).astype(jnp.int32)
    vmem = pl.BlockSpec(memory_space=pltpu.VMEM)
    operands = [scalars, *queries, *pieces] + ([] if first else list(totals))
    scratch = [
        pltpu.VMEM((n_q, rows, width), jnp.bfloat16),
        pltpu.VMEM((n_kv, rows, pieces[0].shape[1]), jnp.bfloat16),
    ]
    aliases = {}
    if last:
        out_shape = [jax.ShapeDtypeStruct((rows, width), jnp.bfloat16)] * n_q
        scratch += [
            pltpu.VMEM(acc_shape.shape, jnp.float32),
            pltpu.VMEM(den_shape.shape, jnp.float32),
        ]
    else:
        out_shape = [acc_shape, den_shape]
        if not first:
            aliases = {1 + n_q + n_kv: 0, 2 + n_q + n_kv: 1}
    flops = n_q * n_kv * heads * 4 * rows * rows * HD * 2 // 3
    return pl.pallas_call(
        functools.partial(attend_kernel, n_q, n_kv, WINDOW // rows, first, last),
        out_shape=out_shape,
        in_specs=[pl.BlockSpec(memory_space=pltpu.SMEM)] + [vmem] * (len(operands) - 1),
        out_specs=[vmem] * len(out_shape),
        scratch_shapes=scratch,
        input_output_aliases=aliases,
        compiler_params=pltpu.CompilerParams(vmem_limit_bytes=24 * 1024 * 1024),
        cost_estimate=pl.CostEstimate(
            flops=flops,
            bytes_accessed=n_q * rows * width * 10,
            transcendentals=2 * n_q * n_kv * heads * rows * rows,
        ),
    )(*operands)


def local(tokens, pre_gain, query_weight, key_weight, value_weight, out_weight, post_gain):
    n_seq = lax.axis_size("seq")
    cores = lax.axis_size("head")
    rows, part = tokens.shape
    kv_heads = key_weight.shape[1] // HD
    query_heads = query_weight.shape[1] // HD
    piece_width = query_heads // kv_heads * HD
    plane = cores * kv_heads
    hops = WINDOW // (rows * plane)
    seq = lax.axis_index("seq")
    core = lax.axis_index("head")
    place = seq % plane
    column = place % kv_heads
    row = place // kv_heads

    def over_cores(value, by=1):
        return lax.ppermute(value, "head", [(c, (c + by) % cores) for c in range(cores)])

    def next_plane(value):
        return lax.ppermute(value, "seq", [(i, i + plane) for i in range(n_seq - plane)])

    def route(turn):
        pairs = []
        for s in range(n_seq):
            base, at = s - s % plane, s % plane
            y, x = at // kv_heads, at % kv_heads
            for c in range(cores):
                target = base + c * kv_heads + (x + c + turn) % kv_heads
                pairs.append((s * cores + c, target * cores + y))
        return pairs

    def spread(value, turn):
        return lax.ppermute(value, ("seq", "head"), route(turn))

    def gather_back(value, turn):
        return lax.ppermute(value, ("seq", "head"), [(b, a) for a, b in route(turn)])

    turns = range(kv_heads)
    others = range(1, cores)

    def held_by(c, turn):
        return (column + c + turn) % kv_heads

    shards = [tokens] + [over_cores(tokens, by) for by in others]
    firsts = [(core - by) % cores * part for by in range(cores)]
    positions = seq * rows + jnp.arange(rows, dtype=jnp.int32)
    tables = rope_tables(positions, HD)
    kv_block = ((0, HD, True), (1, HD, False))
    kv_weights = [key_weight, value_weight]
    sent = []
    source = (shards, firsts, pre_gain)
    for turn in turns:
        start = held_by(core, turn) * HD
        out = project(source, tables, kv_weights, (kv_block,), [start, start])
        if turn == 0:
            source, out = out[0], out[1:]
        sent.append(out[0])
    q_out = project(
        source,
        tables,
        [query_weight],
        (((0, piece_width, True),),) * kv_heads,
        [held_by(core, turn) * piece_width for turn in turns],
    )

    travelling = [next_plane(piece) for piece in sent]
    q_pieces = [spread(piece, turn) for turn, piece in enumerate(q_out)]
    levels = [[spread(piece, turn) for turn, piece in enumerate(sent)]]
    level = [spread(piece, turn) for turn, piece in enumerate(travelling)]
    levels.append(level)
    for _ in range(1, hops):
        level = [next_plane(piece) for piece in level]
        levels.append(level)

    group_base = seq - place
    block_at = [(column - row - turn) % kv_heads for turn in turns]
    query_blocks = [group_base + core * kv_heads + block_at[turn] for turn in turns]

    def merged(level, lag, some):
        pieces, blocks = [], []
        for turn in some:
            for by in range(cores):
                piece = level[turn] if by == 0 else over_cores(level[turn], by)
                origin = (core - by) % cores
                pieces.append(piece)
                blocks.append(group_base - lag * plane + origin * kv_heads + block_at[turn])
        return pieces, blocks

    totals = None
    for lag, level in enumerate(levels):
        split = [turns] if lag == 0 else [[turn] for turn in turns]
        for index, some in enumerate(split):
            pieces, blocks = merged(level, lag, some)
            last = lag == len(levels) - 1 and index == len(split) - 1
            totals = attend(query_blocks, blocks, q_pieces, pieces, totals, last)

    zero = jnp.zeros((), jnp.int32)
    row_blocks = [out_weight]
    for by in others:
        target = (core + by) % cores
        block = lax.dynamic_slice_in_dim(out_weight, target * part, part, 1)
        row_blocks.append(over_cores(block, by))
    total = None
    for turn, o in enumerate(totals):
        own = gather_back(o, turn)
        lefts = [own] + [over_cores(own, by) for by in others]
        starts = []
        for by in range(cores):
            starts.append(held_by((core - by) % cores, turn) * piece_width)
            starts.append(core * part if by == 0 else zero)
        out = out_project(lefts, row_blocks, starts, total, turn == kv_heads - 1)
        total = out[0]
    share, squares = out
    squares = squares.reshape(rows)
    total_square = squares
    for by in others:
        total_square = total_square + over_cores(squares, by)
    inverse_rms = lax.rsqrt(total_square / (part * cores) + norm_epsilon)[:, None]
    return (tokens.astype(jnp.float32) + post_gain * share * inverse_rms).astype(jnp.bfloat16)


def solution(mesh):
    placed = (
        P("seq", "head"),
        P(),
        P(None, "head"),
        P(None, "head"),
        P(None, "head"),
        P("head", None),
        P("head"),
    )
    return jax.shard_map(
        local, mesh=mesh, in_specs=placed, out_specs=P("seq", "head"), check_vma=False
    )
```

```python
import functools

import jax
import jax.numpy as jnp
from jax import lax
from jax.experimental import pallas as pl
from jax.experimental.pallas import tpu as pltpu
from jax.sharding import PartitionSpec as P


HD = 256
WINDOW = 4096

softcap_limit = 50.0
rope_base = 10000.0
norm_epsilon = 1e-06


LOG2E = 1.4426950408889634
ROW_CHUNK = 256


def rope_tables(positions, head_dim):
    midpoint = head_dim // 2
    frequency = jnp.exp(
        -jnp.log(rope_base) * (2.0 * jnp.arange(midpoint, dtype=jnp.float32) / head_dim)
    )
    angles = positions.astype(jnp.float32)[:, None] * frequency[None, :]
    return jnp.cos(angles), jnp.sin(angles)


def dot(left, right):
    return jnp.dot(left, right, preferred_element_type=jnp.float32)


VMEM = pl.BlockSpec(memory_space=pltpu.VMEM)
SMEM = pl.BlockSpec(memory_space=pltpu.SMEM)
FAR = pl.BlockSpec(memory_space=pltpu.HBM)
MIB = 1024 * 1024
GRANT = 8
SLOW = 10**11


class Fetch:
    def __init__(self, arrays, outputs):
        self.arrays = arrays
        self.outputs = outputs
        self.plan = [(k, *block) for k, (_, blocks) in enumerate(outputs) for block in blocks]

    def shapes(self):
        return [jax.ShapeDtypeStruct(shape, jnp.bfloat16) for shape, _ in self.outputs]

    def scratch(self):
        return [pltpu.SemaphoreType.DMA((len(self.plan),))] if self.plan else []

    def start(self, numbers, arrays, outputs, arrived):
        copies = []
        for k, (index, array, row, column, shape, *starts) in enumerate(self.plan):
            source = []
            for start, size in zip(starts, shape):
                first = start or 0
                if callable(first):
                    first = pl.multiple_of(first(numbers), size)
                source.append(pl.ds(first, size))
            copy = pltpu.make_async_copy(
                arrays[array].at[source[0], source[1]],
                outputs[index].at[pl.ds(row, shape[0]), pl.ds(column, shape[1])],
                arrived.at[k],
            )
            copy.start()
            copies.append(copy)
        return copies


def kernel_call(body, fetch, numbers, operands, out_shape, scratch, grant, flops, aliases=None):
    n_operands, n_arrays = len(operands), len(fetch.arrays)
    n_out, n_fetched = len(out_shape), len(fetch.outputs)

    def kernel(numbers_ref, *refs):
        refs = list(refs)
        inputs, refs = refs[:n_operands], refs[n_operands:]
        arrays, refs = refs[:n_arrays], refs[n_arrays:]
        outputs, refs = refs[:n_out], refs[n_out:]
        fetched, refs = refs[:n_fetched], refs[n_fetched:]
        copies = []
        if fetch.plan:
            copies = fetch.start(numbers_ref, arrays, fetched, refs[-1])
            refs = refs[:-1]
        body(numbers_ref, inputs, outputs, refs)
        for copy in copies:
            copy.wait()

    moved = sum(x.size * x.dtype.itemsize for x in (*operands, *out_shape))
    return pl.pallas_call(
        kernel,
        out_shape=list(out_shape) + fetch.shapes(),
        in_specs=[SMEM] + [VMEM] * n_operands + [FAR] * n_arrays,
        out_specs=[VMEM] * (n_out + n_fetched),
        scratch_shapes=list(scratch) + fetch.scratch(),
        input_output_aliases={1 + i: o for i, o in (aliases or {}).items()},
        compiler_params=pltpu.CompilerParams(vmem_limit_bytes=grant * MIB),
        cost_estimate=pl.CostEstimate(flops=flops, bytes_accessed=moved, transcendentals=0),
    )(numbers, *operands, *fetch.arrays)


NOTHING = Fetch([], [])


def lane_sums(value, lanes):
    part = value[:, :lanes]
    for k in range(lanes, value.shape[1], lanes):
        part = part + value[:, k : k + lanes]
    return part


def sum_squares(numbers, tokens, ready, fetch):
    rows, part = tokens.shape
    lanes = min(128, part)

    def body(scalars, inputs, outputs, scratch):
        step = min(16, rows)

        def some_rows(t, carry):
            at = pl.ds(pl.multiple_of(t * step, step), step)
            total = None
            for k in range(0, part, lanes):
                value = inputs[0][at, k : k + lanes].astype(jnp.float32)
                value = value * value
                total = value if total is None else total + value
            outputs[0][at, :] = total
            return carry

        lax.fori_loop(0, rows // step, some_rows, 0, unroll=2)

    out = [jax.ShapeDtypeStruct((rows, lanes), jnp.float32)]
    return kernel_call(body, fetch, numbers, [tokens, *ready], out, [], 6, SLOW)


def write_blocks(numbers, normed, firsts, weight_refs, blocks, tables, out_ref):
    cosine, sine_part = tables
    column = 0
    for weight, width, first, turned in blocks:
        here = pl.ds(pl.multiple_of(first(numbers), width), width)
        product = None
        part = normed.shape[1] // len(firsts)
        for k, start in enumerate(firsts):
            deep = pl.ds(pl.multiple_of(start(numbers), part), part)
            term = dot(normed[:, k * part : (k + 1) * part], weight_refs[weight][deep, here])
            product = term if product is None else product + term
        for head in range(0, width, HD):
            middle, end = head + HD // 2, head + HD
            leading, trailing = product[:, head:middle], product[:, middle:end]
            if turned:
                cos, sin = cosine[...], sine_part[...]
                leading, trailing = leading * cos - trailing * sin, trailing * cos + leading * sin
            out_ref[:, column + head : column + middle] = leading.astype(jnp.bfloat16)
            out_ref[:, column + middle : column + end] = trailing.astype(jnp.bfloat16)
        column += width


def normed_projection(
    numbers, shards, firsts, gain, squares, tables, weights, blocks, fetch
):
    n = len(shards)
    rows, part = shards[0].shape

    def body(scalars, inputs, outputs, scratch):
        shard_refs, square_refs = inputs[:n], inputs[n : 2 * n]
        gain_ref, cosine, sine_part = inputs[2 * n : 2 * n + 3]
        weight_refs = inputs[2 * n + 3 :]
        normed, out_ref = outputs
        scale_ref = scratch[0]
        total = square_refs[0][...]
        for ref in square_refs[1:]:
            total = total + ref[...]
        total = jnp.sum(total, axis=-1, keepdims=True)
        scale = lax.rsqrt(total / (part * n) + norm_epsilon)
        scale_ref[...] = jnp.broadcast_to(scale, scale_ref.shape)
        gains = scratch[1]
        step = gains.shape[0]
        lanes = scale_ref.shape[1]
        for k in range(n):
            first = firsts[k](scalars)
            for column in range(0, part, lanes):
                gain = gain_ref[pl.ds((first + column) // lanes, 1), :]
                here = slice(k * part + column, k * part + column + lanes)
                gains[:, here] = jnp.broadcast_to(gain, (step, lanes))

        def norm_rows(t, carry):
            at = pl.ds(pl.multiple_of(t * step, step), step)
            scale = scale_ref[at, :]
            for k, shard in enumerate(shard_refs):
                for column in range(0, part, lanes):
                    here = slice(k * part + column, k * part + column + lanes)
                    value = shard[at, column : column + lanes].astype(jnp.float32)
                    value = value * scale * gains[:, here]
                    normed[at, here] = value.astype(jnp.bfloat16)
            return carry

        lax.fori_loop(0, rows // step, norm_rows, 0, unroll=2)
        write_blocks(scalars, normed, firsts, weight_refs, blocks, (cosine, sine_part), out_ref)

    width = sum(width for _, width, _, _ in blocks)
    out = [
        jax.ShapeDtypeStruct((rows, part * n), jnp.bfloat16),
        jax.ShapeDtypeStruct((rows, width), jnp.bfloat16),
    ]
    operands = [*shards, *squares, gain, *tables, *weights]
    flops = 2 * rows * part * n * width
    scratch = [
        pltpu.VMEM((rows, min(128, part)), jnp.float32),
        pltpu.VMEM((min(16, rows), part * n), jnp.float32),
    ]
    return kernel_call(body, fetch, numbers, operands, out, scratch, GRANT, flops)


def projection(numbers, normed, firsts, tables, weights, outputs, fetch):
    rows = normed.shape[0]

    def body(scalars, inputs, outs, scratch):
        for blocks, out_ref in zip(outputs, outs):
            write_blocks(
                scalars, inputs[0], firsts, inputs[3:], blocks, inputs[1:3], out_ref
            )

    widths = [sum(width for _, width, _, _ in blocks) for blocks in outputs]
    out = [jax.ShapeDtypeStruct((rows, width), jnp.bfloat16) for width in widths]
    flops = 2 * normed.size * sum(widths)
    return kernel_call(body, fetch, numbers, [normed, *tables, *weights], out, [], 8, flops)


def out_projection(numbers, lefts, weight, total, last):
    n = len(lefts)
    rows, width = lefts[0].shape
    out_width = weight.shape[1]
    lanes = min(128, out_width)
    columns = 256 if out_width % 256 == 0 else out_width

    def body(scalars, inputs, outputs, scratch):
        weight_ref = inputs[n]
        left = scratch[0]
        for k in range(n):
            left[:, k * width : (k + 1) * width] = inputs[k][...]
        for column in range(0, out_width, columns):
            here = slice(column, column + columns)
            value = dot(left[...], weight_ref[:, here])
            if total is not None:
                value = value + inputs[n + 1][:, here]
            outputs[0][:, here] = value
            if last:
                part = lane_sums(value * value, lanes)
                if column == 0:
                    outputs[1][...] = part
                else:
                    outputs[1][...] = outputs[1][...] + part

    out = [jax.ShapeDtypeStruct((rows, out_width), jnp.float32)]
    if last:
        out.append(jax.ShapeDtypeStruct((rows, lanes), jnp.float32))
    operands = [*lefts, weight] + ([] if total is None else [total])
    aliases = {} if total is None else {n + 1: 0}
    scratch = [pltpu.VMEM((rows, n * width), jnp.bfloat16)]
    flops = 2 * rows * n * width * out_width
    return kernel_call(body, NOTHING, numbers, operands, out, scratch, 8, flops, aliases)


def finish_kernel(n, tokens, share, gain, *refs):
    square_refs, out, scale_ref = refs[:n], refs[n], refs[n + 1]
    block, part = out.shape
    lanes = scale_ref.shape[1]
    base = pl.program_id(0) * block
    at = pl.ds(pl.multiple_of(base, block), block)
    total = square_refs[0][at, :]
    for ref in square_refs[1:]:
        total = total + ref[at, :]
    total = jnp.sum(total, axis=-1, keepdims=True)
    scale = lax.rsqrt(total / (part * n) + norm_epsilon)
    scale_ref[...] = jnp.broadcast_to(scale, scale_ref.shape)
    step = min(16, block)

    def some_rows(t, carry):
        here = pl.ds(pl.multiple_of(t * step, step), step)
        at = pl.ds(pl.multiple_of(base + t * step, step), step)
        scale = scale_ref[here, :]
        for column in range(0, part, lanes):
            columns = slice(column, column + lanes)
            value = gain[column // lanes : column // lanes + 1, :] * share[at, columns] * scale
            value = tokens[at, columns].astype(jnp.float32) + value
            out[here, columns] = value.astype(jnp.bfloat16)
        return carry

    lax.fori_loop(0, block // step, some_rows, 0, unroll=2)


def finish(tokens, share, gain, squares):
    rows, part = tokens.shape
    step = min(128, rows)
    return pl.pallas_call(
        functools.partial(finish_kernel, len(squares)),
        grid=(rows // step,),
        out_shape=jax.ShapeDtypeStruct((rows, part), jnp.bfloat16),
        in_specs=[VMEM] * (3 + len(squares)),
        out_specs=pl.BlockSpec((step, part), lambda t: (t, 0)),
        scratch_shapes=[pltpu.VMEM((step, min(128, part)), jnp.float32)],
        compiler_params=pltpu.CompilerParams(vmem_limit_bytes=8 * MIB),
        cost_estimate=pl.CostEstimate(
            flops=8 * rows * part, bytes_accessed=8 * rows * part, transcendentals=0
        ),
    )(tokens, share, gain, *squares)


def attend(numbers, query_blocks, key_blocks, queries, pieces, totals, last, full, fetch):
    n_q, n_kv = len(queries), len(pieces)
    rows, width = queries[0].shape
    heads = width // HD
    lanes = min(128, rows)
    window_blocks = WINDOW // rows
    first = totals is None
    acc_shape = (n_q, rows, width)
    den_shape = (n_q, rows, heads * lanes)
    chunk = min(ROW_CHUNK, rows)

    def body(scalars, inputs, outputs, scratch):
        q_refs, kv_refs = inputs[:n_q], inputs[n_q : n_q + n_kv]
        kv_all, key_numbers = scratch[:2]
        acc, den = scratch[2:] if last else outputs
        for k in range(n_kv):
            kv_all[k * rows : (k + 1) * rows, :] = kv_refs[k][...]
            key_numbers[k] = key_blocks[k](scalars)
        if first:
            acc[...] = jnp.zeros_like(acc)
            den[...] = jnp.zeros_like(den)
        elif last:
            acc[...] = inputs[n_q + n_kv][...]
            den[...] = inputs[n_q + n_kv + 1][...]

        def add(r, keys_at, delta):
            for head in range(heads):
                for start in range(0, rows, chunk):
                    at = slice(start, start + chunk)
                    columns = slice(head * HD, (head + 1) * HD)
                    scores = lax.dot_general(
                        q_refs[r][at, columns],
                        kv_all[keys_at, :HD],
                        (((1,), (1,)), ((), ())),
                        preferred_element_type=jnp.float32,
                    )
                    weights = jnp.exp2(
                        jnp.tanh(scores * (HD ** (-0.5) / softcap_limit))
                        * (softcap_limit * LOG2E)
                    )
                    if delta is not None:
                        offset = (
                            lax.broadcasted_iota(jnp.int32, weights.shape, 0)
                            - lax.broadcasted_iota(jnp.int32, weights.shape, 1)
                            + (delta * rows + start)
                        )
                        allowed = (offset >= 0) & (offset < window_blocks * rows)
                        weights = jnp.where(allowed, weights, 0.0)
                    lane_at = slice(head * lanes, (head + 1) * lanes)
                    den[r, at, lane_at] = den[r, at, lane_at] + lane_sums(weights, lanes)
                    acc[r, at, columns] = acc[r, at, columns] + dot(
                        weights.astype(jnp.bfloat16), kv_all[keys_at, HD:]
                    )

        if full:

            @pl.when(key_numbers[0] >= 0)
            def _():
                for r in range(n_q):
                    add(r, slice(0, n_kv * rows), None)

        else:

            def step(n, carry):
                key_block = key_numbers[n]
                live = key_block >= 0
                deltas = [block(scalars) - key_block for block in query_blocks]
                inside = [(delta > 0) & (delta < window_blocks) for delta in deltas]
                every = functools.reduce(jnp.logical_and, inside)
                keys_at = pl.ds(pl.multiple_of(n * rows, rows), rows)

                @pl.when(live & every)
                def _():
                    for r in range(n_q):
                        add(r, keys_at, None)

                for r in range(n_q):
                    some = (deltas[r] >= 0) & (deltas[r] <= window_blocks)

                    @pl.when(live & some & jnp.logical_not(every))
                    def _():
                        add(r, keys_at, deltas[r])

                return carry

            lax.fori_loop(0, n_kv, step, 0)
        if last:
            for r in range(n_q):
                for head in range(heads):
                    total = jnp.sum(
                        den[r, :, head * lanes : (head + 1) * lanes], axis=-1, keepdims=True
                    )
                    columns = slice(head * HD, (head + 1) * HD)
                    outputs[r][:, columns] = (acc[r, :, columns] / total).astype(jnp.bfloat16)

    scratch = [
        pltpu.VMEM((n_kv * rows, pieces[0].shape[1]), jnp.bfloat16),
        pltpu.SMEM((n_kv,), jnp.int32),
    ]
    operands = [*queries, *pieces] + ([] if first else list(totals))
    aliases = {}
    if last:
        out = [jax.ShapeDtypeStruct((rows, width), jnp.bfloat16)] * n_q
        scratch += [pltpu.VMEM(acc_shape, jnp.float32), pltpu.VMEM(den_shape, jnp.float32)]
    else:
        out = [
            jax.ShapeDtypeStruct(acc_shape, jnp.float32),
            jax.ShapeDtypeStruct(den_shape, jnp.float32),
        ]
        if not first:
            aliases = {n_q + n_kv: 0, n_q + n_kv + 1: 1}
    flops = n_q * n_kv * heads * 4 * rows * rows * HD * 2 // 3
    return kernel_call(body, fetch, numbers, operands, out, scratch, 14, flops, aliases)


def local(tokens, pre_gain, query_weight, key_weight, value_weight, out_weight, post_gain):
    n_seq = lax.axis_size("seq")
    cores = lax.axis_size("head")
    rows, part = tokens.shape
    kv_heads = key_weight.shape[1] // HD
    query_heads = query_weight.shape[1] // HD
    piece_width = query_heads // kv_heads * HD
    plane = cores * kv_heads
    hops = WINDOW // (rows * plane)
    seq = lax.axis_index("seq")
    core = lax.axis_index("head")
    place = seq % plane
    column = place % kv_heads
    row = place // kv_heads

    def over_cores(value, by=1):
        return lax.ppermute(value, "head", [(c, (c + by) % cores) for c in range(cores)])

    def next_plane(value):
        return lax.ppermute(value, "seq", [(i, i + plane) for i in range(n_seq - plane)])

    def route(turn):
        pairs = []
        for s in range(n_seq):
            base, at = s - s % plane, s % plane
            y, x = at // kv_heads, at % kv_heads
            for c in range(cores):
                target = base + c * kv_heads + (x + c + turn) % kv_heads
                pairs.append((s * cores + c, target * cores + y))
        return pairs

    def spread(value, turn):
        return lax.ppermute(value, ("seq", "head"), route(turn))

    def gather_back(value, turn):
        return lax.ppermute(value, ("seq", "head"), [(b, a) for a, b in route(turn)])

    turns = range(kv_heads)
    others = range(1, cores)
    numbers = jnp.stack([core, column, row, seq - place]).astype(jnp.int32)

    def held_by(by, turn, scale):
        def start(ref):
            return lax.rem(ref[1] + lax.rem(ref[0] + cores - by, cores) + turn, kv_heads) * scale

        return start

    shards = [tokens] + [over_cores(tokens, by) for by in others]
    firsts = [
        (lambda ref, by=by: lax.rem(ref[0] + cores - by, cores) * part) for by in range(cores)
    ]
    positions = seq * rows + jnp.arange(rows, dtype=jnp.int32)
    tables = rope_tables(positions, HD)
    lanes = min(128, part)
    gain_in, gain_out = pre_gain.reshape(-1, lanes), post_gain.reshape(-1, lanes)
    (own_squares,) = sum_squares(numbers, tokens, [*tables, gain_in, gain_out], NOTHING)
    kv_weights = [key_weight, value_weight]
    squares = [own_squares] + [over_cores(own_squares, by) for by in others]
    kv_blocks = [
        [(n, HD, held_by(0, turn, HD), n == 0) for n in range(len(kv_weights))] for turn in turns
    ]
    q_blocks = [[(0, piece_width, held_by(0, turn, piece_width), True)] for turn in turns]
    normed, piece = normed_projection(
        numbers,
        shards,
        firsts,
        gain_in,
        squares,
        tables,
        kv_weights,
        kv_blocks[0],
        NOTHING,
    )
    sent = [piece]
    row_blocks = [out_weight]
    out_rows = out_weight.shape[0]
    for turn in turns[1:]:
        fetch = NOTHING
        if turn == 1:
            shape = (out_rows, part)
            columns = [
                (lambda ref, by=by: lax.rem(ref[0] + by, cores) * part) for by in others
            ]
            fetch = Fetch(
                [out_weight], [(shape, [(0, 0, 0, shape, None, first)]) for first in columns]
            )
        piece, *blocks = projection(
            numbers, normed, firsts, tables, kv_weights, [kv_blocks[turn]], fetch
        )
        sent.append(piece)
        row_blocks += [over_cores(block, by) for by, block in zip(others, blocks)]
    q_out = []
    for turn in turns:
        q_out += projection(
            numbers, normed, firsts, tables, [query_weight], [q_blocks[turn]], NOTHING
        )

    travelling = [next_plane(piece) for piece in sent]
    q_pieces = [spread(piece, turn) for turn, piece in enumerate(q_out)]
    levels = [[spread(piece, turn) for turn, piece in enumerate(sent)]]
    level = [spread(piece, turn) for turn, piece in enumerate(travelling)]
    levels.append(level)
    for _ in range(2, hops + 1):
        level = [next_plane(piece) for piece in level]
        levels.append(level)

    def block_of(by, turn, lag):
        def block(ref):
            column_of = lax.rem(ref[1] - ref[2] - turn + cores * plane * kv_heads, kv_heads)
            row_of = lax.rem(ref[0] + cores - by, cores)
            return ref[3] - lag * plane + row_of * kv_heads + column_of

        return block

    query_blocks = [block_of(0, turn, 0) for turn in turns]

    def piece_of(lag, turn, by):
        piece = levels[lag][turn]
        return over_cores(piece, by) if by else piece

    out_fetch = []
    for turn in turns:
        blocks = []
        for by in range(cores):
            blocks.append(
                (
                    by,
                    by * piece_width,
                    0,
                    (piece_width, part),
                    held_by(by, turn, piece_width),
                    None if by else (lambda ref: ref[0] * part),
                )
            )
        out_fetch.append(((piece_width * cores, part), blocks))
    calls = []
    for lag in range(1, hops + 1):
        for turn in turns:
            calls.append([(lag, turn, by) for by in range(cores)])
        if lag == 1:
            calls += [[(0, turn, by) for by in range(cores)] for turn in turns]
    calls[-1:] = [calls[-1][:1], calls[-1][1:]]
    totals = None
    for index, call in enumerate(calls):
        blocks = [block_of(by, turn, lag) for lag, turn, by in call]
        pieces = [piece_of(*key) for key in call]
        last = index == len(calls) - 1
        full = all(0 < lag < hops for lag, _, _ in call)
        fetch = Fetch(row_blocks, out_fetch) if index == len(calls) - 3 else NOTHING
        totals = attend(numbers, query_blocks, blocks, q_pieces, pieces, totals, last, full, fetch)
        if fetch is not NOTHING:
            totals, out_blocks = totals[:2], totals[2:]
    attended = totals
    total = None
    for turn, o in enumerate(attended):
        own = gather_back(o, turn)
        lefts = [own] + [over_cores(own, by) for by in others]
        out = out_projection(numbers, lefts, out_blocks[turn], total, turn == kv_heads - 1)
        total = out[0]
    share, own_squares = out
    squares = [own_squares] + [over_cores(own_squares, by) for by in others]
    return finish(tokens, share, gain_out, squares)


def solution(mesh):
    placed = (
        P("seq", "head"),
        P(),
        P(None, "head"),
        P(None, "head"),
        P(None, "head"),
        P("head", None),
        P("head"),
    )
    return jax.shard_map(
        local, mesh=mesh, in_specs=placed, out_specs=P("seq", "head"), check_vma=False
    )
```

```python
import functools

import jax
import jax.numpy as jnp
from jax import lax
from jax.experimental import pallas as pl
from jax.experimental.pallas import tpu as pltpu
from jax.sharding import PartitionSpec as P


HD = 256
WINDOW = 4096

softcap_limit = 50.0
rope_base = 10000.0
norm_epsilon = 1e-06


LOG2E = 1.4426950408889634
ROW_CHUNK = 256


def rope_tables(positions, head_dim):
    midpoint = head_dim // 2
    frequency = jnp.exp(
        -jnp.log(rope_base) * (2.0 * jnp.arange(midpoint, dtype=jnp.float32) / head_dim)
    )
    angles = positions.astype(jnp.float32)[:, None] * frequency[None, :]
    return jnp.cos(angles), jnp.sin(angles)


def dot(left, right):
    return jnp.dot(left, right, preferred_element_type=jnp.float32)


VMEM = pl.BlockSpec(memory_space=pltpu.VMEM)
SMEM = pl.BlockSpec(memory_space=pltpu.SMEM)
FAR = pl.BlockSpec(memory_space=pltpu.HBM)
MIB = 1024 * 1024
GRANT = 8
SLOW = 10**11


class Fetch:
    def __init__(self, arrays, outputs):
        self.arrays = arrays
        self.outputs = outputs
        self.plan = [(k, *block) for k, (_, blocks) in enumerate(outputs) for block in blocks]

    def shapes(self):
        return [jax.ShapeDtypeStruct(shape, jnp.bfloat16) for shape, _ in self.outputs]

    def scratch(self):
        return [pltpu.SemaphoreType.DMA((len(self.plan),))] if self.plan else []

    def start(self, numbers, arrays, outputs, arrived):
        copies = []
        for k, (index, array, row, column, shape, *starts) in enumerate(self.plan):
            source = []
            for start, size in zip(starts, shape):
                first = start or 0
                if callable(first):
                    first = pl.multiple_of(first(numbers), size)
                source.append(pl.ds(first, size))
            copy = pltpu.make_async_copy(
                arrays[array].at[source[0], source[1]],
                outputs[index].at[pl.ds(row, shape[0]), pl.ds(column, shape[1])],
                arrived.at[k],
            )
            copy.start()
            copies.append(copy)
        return copies


def kernel_call(body, fetch, numbers, operands, out_shape, scratch, grant, flops, aliases=None):
    n_operands, n_arrays = len(operands), len(fetch.arrays)
    n_out, n_fetched = len(out_shape), len(fetch.outputs)

    def kernel(numbers_ref, *refs):
        refs = list(refs)
        inputs, refs = refs[:n_operands], refs[n_operands:]
        arrays, refs = refs[:n_arrays], refs[n_arrays:]
        outputs, refs = refs[:n_out], refs[n_out:]
        fetched, refs = refs[:n_fetched], refs[n_fetched:]
        copies = []
        if fetch.plan:
            copies = fetch.start(numbers_ref, arrays, fetched, refs[-1])
            refs = refs[:-1]
        body(numbers_ref, inputs, outputs, refs)
        for copy in copies:
            copy.wait()

    moved = sum(x.size * x.dtype.itemsize for x in (*operands, *out_shape))
    return pl.pallas_call(
        kernel,
        out_shape=list(out_shape) + fetch.shapes(),
        in_specs=[SMEM] + [VMEM] * n_operands + [FAR] * n_arrays,
        out_specs=[VMEM] * (n_out + n_fetched),
        scratch_shapes=list(scratch) + fetch.scratch(),
        input_output_aliases={1 + i: o for i, o in (aliases or {}).items()},
        compiler_params=pltpu.CompilerParams(vmem_limit_bytes=grant * MIB),
        cost_estimate=pl.CostEstimate(flops=flops, bytes_accessed=moved, transcendentals=0),
    )(numbers, *operands, *fetch.arrays)


NOTHING = Fetch([], [])


def lane_sums(value, lanes):
    part = value[:, :lanes]
    for k in range(lanes, value.shape[1], lanes):
        part = part + value[:, k : k + lanes]
    return part


def sum_squares(numbers, tokens, ready, fetch):
    rows, part = tokens.shape
    lanes = min(128, part)

    def body(scalars, inputs, outputs, scratch):
        step = min(16, rows)

        def some_rows(t, carry):
            at = pl.ds(pl.multiple_of(t * step, step), step)
            total = None
            for k in range(0, part, lanes):
                value = inputs[0][at, k : k + lanes].astype(jnp.float32)
                value = value * value
                total = value if total is None else total + value
            outputs[0][at, :] = total
            return carry

        lax.fori_loop(0, rows // step, some_rows, 0, unroll=2)

    out = [jax.ShapeDtypeStruct((rows, lanes), jnp.float32)]
    return kernel_call(body, fetch, numbers, [tokens, *ready], out, [], 6, SLOW)


def write_blocks(numbers, normed, firsts, weight_refs, blocks, tables, out_ref):
    cosine, sine_part = tables
    column = 0
    for weight, width, first, turned in blocks:
        here = pl.ds(pl.multiple_of(first(numbers), width), width)
        product = None
        part = normed.shape[1] // len(firsts)
        for k, start in enumerate(firsts):
            deep = pl.ds(pl.multiple_of(start(numbers), part), part)
            term = dot(normed[:, k * part : (k + 1) * part], weight_refs[weight][deep, here])
            product = term if product is None else product + term
        for head in range(0, width, HD):
            middle, end = head + HD // 2, head + HD
            leading, trailing = product[:, head:middle], product[:, middle:end]
            if turned:
                cos, sin = cosine[...], sine_part[...]
                leading, trailing = leading * cos - trailing * sin, trailing * cos + leading * sin
            out_ref[:, column + head : column + middle] = leading.astype(jnp.bfloat16)
            out_ref[:, column + middle : column + end] = trailing.astype(jnp.bfloat16)
        column += width


def normed_projection(
    numbers, shards, firsts, gain, squares, tables, weights, blocks, fetch
):
    n = len(shards)
    rows, part = shards[0].shape

    def body(scalars, inputs, outputs, scratch):
        shard_refs, square_refs = inputs[:n], inputs[n : 2 * n]
        gain_ref, cosine, sine_part = inputs[2 * n : 2 * n + 3]
        weight_refs = inputs[2 * n + 3 :]
        normed, out_ref = outputs
        scale_ref = scratch[0]
        total = square_refs[0][...]
        for ref in square_refs[1:]:
            total = total + ref[...]
        total = jnp.sum(total, axis=-1, keepdims=True)
        scale = lax.rsqrt(total / (part * n) + norm_epsilon)
        scale_ref[...] = jnp.broadcast_to(scale, scale_ref.shape)
        gains = scratch[1]
        step = gains.shape[0]
        lanes = scale_ref.shape[1]
        for k in range(n):
            first = firsts[k](scalars)
            for column in range(0, part, lanes):
                gain = gain_ref[pl.ds((first + column) // lanes, 1), :]
                here = slice(k * part + column, k * part + column + lanes)
                gains[:, here] = jnp.broadcast_to(gain, (step, lanes))

        def norm_rows(t, carry):
            at = pl.ds(pl.multiple_of(t * step, step), step)
            scale = scale_ref[at, :]
            for k, shard in enumerate(shard_refs):
                for column in range(0, part, lanes):
                    here = slice(k * part + column, k * part + column + lanes)
                    value = shard[at, column : column + lanes].astype(jnp.float32)
                    value = value * scale * gains[:, here]
                    normed[at, here] = value.astype(jnp.bfloat16)
            return carry

        lax.fori_loop(0, rows // step, norm_rows, 0, unroll=2)
        write_blocks(scalars, normed, firsts, weight_refs, blocks, (cosine, sine_part), out_ref)

    width = sum(width for _, width, _, _ in blocks)
    out = [
        jax.ShapeDtypeStruct((rows, part * n), jnp.bfloat16),
        jax.ShapeDtypeStruct((rows, width), jnp.bfloat16),
    ]
    operands = [*shards, *squares, gain, *tables, *weights]
    flops = 2 * rows * part * n * width
    scratch = [
        pltpu.VMEM((rows, min(128, part)), jnp.float32),
        pltpu.VMEM((min(16, rows), part * n), jnp.float32),
    ]
    return kernel_call(body, fetch, numbers, operands, out, scratch, GRANT, flops)


def projection(numbers, normed, firsts, tables, weights, outputs, fetch):
    rows = normed.shape[0]

    def body(scalars, inputs, outs, scratch):
        for blocks, out_ref in zip(outputs, outs):
            write_blocks(
                scalars, inputs[0], firsts, inputs[3:], blocks, inputs[1:3], out_ref
            )

    widths = [sum(width for _, width, _, _ in blocks) for blocks in outputs]
    out = [jax.ShapeDtypeStruct((rows, width), jnp.bfloat16) for width in widths]
    flops = 2 * normed.size * sum(widths)
    return kernel_call(body, fetch, numbers, [normed, *tables, *weights], out, [], 8, flops)


def out_projection(numbers, lefts, weight, some, total, last):
    n = len(lefts)
    rows, width = lefts[0].shape
    out_width = weight.shape[1]
    lanes = min(128, out_width)
    columns = 256 if out_width % 256 == 0 else out_width

    def body(scalars, inputs, outputs, scratch):
        weight_ref = inputs[n]
        left = scratch[0]
        for k in range(n):
            left[:, k * width : (k + 1) * width] = inputs[k][...]
        for column in range(0, out_width, columns):
            here = slice(column, column + columns)
            value = dot(left[...], weight_ref[some[0] * width : (some[-1] + 1) * width, here])
            if total is not None:
                value = value + inputs[n + 1][:, here]
            outputs[0][:, here] = value
            if last:
                part = lane_sums(value * value, lanes)
                if column == 0:
                    outputs[1][...] = part
                else:
                    outputs[1][...] = outputs[1][...] + part

    out = [jax.ShapeDtypeStruct((rows, out_width), jnp.float32)]
    if last:
        out.append(jax.ShapeDtypeStruct((rows, lanes), jnp.float32))
    operands = [*lefts, weight] + ([] if total is None else [total])
    aliases = {} if total is None else {n + 1: 0}
    scratch = [pltpu.VMEM((rows, n * width), jnp.bfloat16)]
    flops = 2 * rows * n * width * out_width
    return kernel_call(body, NOTHING, numbers, operands, out, scratch, 8, flops, aliases)


def finish_kernel(n, tokens, share, gain, *refs):
    square_refs, out, scale_ref = refs[:n], refs[n], refs[n + 1]
    block, part = out.shape
    lanes = scale_ref.shape[1]
    base = pl.program_id(0) * block
    at = pl.ds(pl.multiple_of(base, block), block)
    total = square_refs[0][at, :]
    for ref in square_refs[1:]:
        total = total + ref[at, :]
    total = jnp.sum(total, axis=-1, keepdims=True)
    scale = lax.rsqrt(total / (part * n) + norm_epsilon)
    scale_ref[...] = jnp.broadcast_to(scale, scale_ref.shape)
    step = min(16, block)

    def some_rows(t, carry):
        here = pl.ds(pl.multiple_of(t * step, step), step)
        at = pl.ds(pl.multiple_of(base + t * step, step), step)
        scale = scale_ref[here, :]
        for column in range(0, part, lanes):
            columns = slice(column, column + lanes)
            value = gain[column // lanes : column // lanes + 1, :] * share[at, columns] * scale
            value = tokens[at, columns].astype(jnp.float32) + value
            out[here, columns] = value.astype(jnp.bfloat16)
        return carry

    lax.fori_loop(0, block // step, some_rows, 0, unroll=2)


def finish(tokens, share, gain, squares):
    rows, part = tokens.shape
    step = min(128, rows)
    return pl.pallas_call(
        functools.partial(finish_kernel, len(squares)),
        grid=(rows // step,),
        out_shape=jax.ShapeDtypeStruct((rows, part), jnp.bfloat16),
        in_specs=[VMEM] * (3 + len(squares)),
        out_specs=pl.BlockSpec((step, part), lambda t: (t, 0)),
        scratch_shapes=[pltpu.VMEM((step, min(128, part)), jnp.float32)],
        compiler_params=pltpu.CompilerParams(vmem_limit_bytes=8 * MIB),
        cost_estimate=pl.CostEstimate(
            flops=8 * rows * part, bytes_accessed=8 * rows * part, transcendentals=0
        ),
    )(tokens, share, gain, *squares)


def attend(numbers, query_blocks, key_blocks, queries, pieces, totals, last, full, fetch):
    n_q, n_kv = len(queries), len(pieces)
    rows, width = queries[0].shape
    heads = width // HD
    lanes = min(128, rows)
    window_blocks = WINDOW // rows
    first = totals is None
    shapes = [(rows, width)] * n_q + [(rows, heads * lanes)] * n_q
    chunk = min(ROW_CHUNK, rows)

    def body(scalars, inputs, outputs, scratch):
        q_refs, kv_refs = inputs[:n_q], inputs[n_q : n_q + n_kv]
        kv_all, key_numbers = scratch[:2]
        state = scratch[2:] if last else outputs
        acc, den = state[:n_q], state[n_q:]
        for k in range(n_kv):
            kv_all[k * rows : (k + 1) * rows, :] = kv_refs[k][...]
            key_numbers[k] = key_blocks[k](scalars)
        for k, ref in enumerate(state):
            if first:
                ref[...] = jnp.zeros_like(ref)
            elif last:
                ref[...] = inputs[n_q + n_kv + k][...]

        def add(r, keys_at, delta):
            for head in range(heads):
                for start in range(0, rows, chunk):
                    at = slice(start, start + chunk)
                    columns = slice(head * HD, (head + 1) * HD)
                    scores = lax.dot_general(
                        q_refs[r][at, columns],
                        kv_all[keys_at, :HD],
                        (((1,), (1,)), ((), ())),
                        preferred_element_type=jnp.float32,
                    )
                    weights = jnp.exp2(
                        jnp.tanh(scores * (HD ** (-0.5) / softcap_limit))
                        * (softcap_limit * LOG2E)
                    )
                    if delta is not None:
                        ahead = (
                            lax.broadcasted_iota(jnp.int32, weights.shape, 0)
                            - lax.broadcasted_iota(jnp.int32, weights.shape, 1)
                            + start
                        )
                        limit = jnp.where((delta > 0) & (delta < window_blocks), -rows, 0)
                        far = delta == window_blocks
                        weights = weights * jnp.where(
                            ahead >= limit,
                            jnp.where(far, 0.0, 1.0).astype(jnp.float32),
                            jnp.where(far, 1.0, 0.0).astype(jnp.float32),
                        )
                    lane_at = slice(head * lanes, (head + 1) * lanes)
                    den[r][at, lane_at] = den[r][at, lane_at] + lane_sums(weights, lanes)
                    acc[r][at, columns] = acc[r][at, columns] + dot(
                        weights.astype(jnp.bfloat16), kv_all[keys_at, HD:]
                    )

        if full:

            @pl.when(key_numbers[0] >= 0)
            def _():
                for r in range(n_q):
                    add(r, slice(0, n_kv * rows), None)

        else:

            def step(n, carry):
                key_block = key_numbers[n]
                live = key_block >= 0
                deltas = [block(scalars) - key_block for block in query_blocks]
                inside = [(delta > 0) & (delta < window_blocks) for delta in deltas]
                every = functools.reduce(jnp.logical_and, inside)
                keys_at = pl.ds(pl.multiple_of(n * rows, rows), rows)

                @pl.when(live & every)
                def _():
                    for r in range(n_q):
                        add(r, keys_at, None)

                for r in range(n_q):
                    some = (deltas[r] >= 0) & (deltas[r] <= window_blocks)

                    @pl.when(live & some & jnp.logical_not(every))
                    def _():
                        add(r, keys_at, deltas[r])

                return carry

            lax.fori_loop(0, n_kv, step, 0)
        if last:
            for r in range(n_q):
                for head in range(heads):
                    total = jnp.sum(
                        den[r][:, head * lanes : (head + 1) * lanes], axis=-1, keepdims=True
                    )
                    columns = slice(head * HD, (head + 1) * HD)
                    outputs[r][:, columns] = (acc[r][:, columns] / total).astype(jnp.bfloat16)

    scratch = [
        pltpu.VMEM((n_kv * rows, pieces[0].shape[1]), jnp.bfloat16),
        pltpu.SMEM((n_kv,), jnp.int32),
    ]
    operands = [*queries, *pieces] + ([] if first else list(totals))
    aliases = {}
    out = [jax.ShapeDtypeStruct(shape, jnp.float32) for shape in shapes]
    if last:
        scratch += [pltpu.VMEM(shape, jnp.float32) for shape in shapes]
        out = [jax.ShapeDtypeStruct((rows, width), jnp.bfloat16)] * n_q
    elif not first:
        aliases = {n_q + n_kv + k: k for k in range(2 * n_q)}
    flops = n_q * n_kv * heads * 4 * rows * rows * HD * 2 // 3
    return kernel_call(body, fetch, numbers, operands, out, scratch, 14, flops, aliases)


def local(tokens, pre_gain, query_weight, key_weight, value_weight, out_weight, post_gain):
    n_seq = lax.axis_size("seq")
    cores = lax.axis_size("head")
    rows, part = tokens.shape
    kv_heads = key_weight.shape[1] // HD
    query_heads = query_weight.shape[1] // HD
    piece_width = query_heads // kv_heads * HD
    plane = cores * kv_heads
    hops = WINDOW // (rows * plane)
    seq = lax.axis_index("seq")
    core = lax.axis_index("head")
    place = seq % plane
    column = place % kv_heads
    row = place // kv_heads

    def over_cores(value, by=1):
        return lax.ppermute(value, "head", [(c, (c + by) % cores) for c in range(cores)])

    def next_plane(value):
        return lax.ppermute(value, "seq", [(i, i + plane) for i in range(n_seq - plane)])

    def route(turn):
        pairs = []
        for s in range(n_seq):
            base, at = s - s % plane, s % plane
            y, x = at // kv_heads, at % kv_heads
            for c in range(cores):
                target = base + c * kv_heads + (x + c + turn) % kv_heads
                pairs.append((s * cores + c, target * cores + y))
        return pairs

    def spread(value, turn):
        return lax.ppermute(value, ("seq", "head"), route(turn))

    def gather_back(value, turn):
        return lax.ppermute(value, ("seq", "head"), [(b, a) for a, b in route(turn)])

    turns = range(kv_heads)
    others = range(1, cores)
    numbers = jnp.stack([core, column, row, seq - place]).astype(jnp.int32)

    def held_by(by, turn, scale):
        def start(ref):
            return lax.rem(ref[1] + lax.rem(ref[0] + cores - by, cores) + turn, kv_heads) * scale

        return start

    shards = [tokens] + [over_cores(tokens, by) for by in others]
    firsts = [
        (lambda ref, by=by: lax.rem(ref[0] + cores - by, cores) * part) for by in range(cores)
    ]
    positions = seq * rows + jnp.arange(rows, dtype=jnp.int32)
    tables = rope_tables(positions, HD)
    lanes = min(128, part)
    gain_in, gain_out = pre_gain.reshape(-1, lanes), post_gain.reshape(-1, lanes)
    (own_squares,) = sum_squares(numbers, tokens, [*tables, gain_in, gain_out], NOTHING)
    kv_weights = [key_weight, value_weight]
    squares = [own_squares] + [over_cores(own_squares, by) for by in others]
    kv_blocks = [
        [(n, HD, held_by(0, turn, HD), n == 0) for n in range(len(kv_weights))] for turn in turns
    ]
    q_blocks = [[(0, piece_width, held_by(0, turn, piece_width), True)] for turn in turns]
    normed, piece = normed_projection(
        numbers,
        shards,
        firsts,
        gain_in,
        squares,
        tables,
        kv_weights,
        kv_blocks[0],
        NOTHING,
    )
    sent = [piece]
    row_blocks = [out_weight]
    out_rows = out_weight.shape[0]
    for turn in turns[1:]:
        fetch = NOTHING
        if turn == 1:
            shape = (out_rows, part)
            columns = [
                (lambda ref, by=by: lax.rem(ref[0] + by, cores) * part) for by in others
            ]
            fetch = Fetch(
                [out_weight], [(shape, [(0, 0, 0, shape, None, first)]) for first in columns]
            )
        piece, *blocks = projection(
            numbers, normed, firsts, tables, kv_weights, [kv_blocks[turn]], fetch
        )
        sent.append(piece)
        row_blocks += [over_cores(block, by) for by, block in zip(others, blocks)]
    q_out = []
    for turn in turns:
        q_out += projection(
            numbers, normed, firsts, tables, [query_weight], [q_blocks[turn]], NOTHING
        )

    travelling = [next_plane(piece) for piece in sent]
    q_pieces = [spread(piece, turn) for turn, piece in enumerate(q_out)]
    levels = [[spread(piece, turn) for turn, piece in enumerate(sent)]]
    level = [spread(piece, turn) for turn, piece in enumerate(travelling)]
    levels.append(level)
    for _ in range(2, hops + 1):
        level = [next_plane(piece) for piece in level]
        levels.append(level)

    def block_of(by, turn, lag):
        def block(ref):
            column_of = lax.rem(ref[1] - ref[2] - turn + cores * plane * kv_heads, kv_heads)
            row_of = lax.rem(ref[0] + cores - by, cores)
            return ref[3] - lag * plane + row_of * kv_heads + column_of

        return block

    query_blocks = [block_of(0, turn, 0) for turn in turns]

    merged = {}

    def piece_of(lag, turn, by):
        if (lag, turn, by) not in merged:
            piece = levels[lag][turn]
            merged[lag, turn, by] = over_cores(piece, by) if by else piece
        return merged[lag, turn, by]

    out_fetch = []
    for turn in turns:
        blocks = []
        for by in range(cores):
            blocks.append(
                (
                    by,
                    by * piece_width,
                    0,
                    (piece_width, part),
                    held_by(by, turn, piece_width),
                    None if by else (lambda ref: ref[0] * part),
                )
            )
        out_fetch.append(((piece_width * cores, part), blocks))
    calls = [[(0, 0, by) for by in range(cores)]]
    for lag in range(1, hops + 1):
        for turn in turns:
            calls.append([(lag, turn, by) for by in range(cores)])
    calls[-1:-1] = [[(0, turn, by) for by in range(cores)] for turn in turns[1:]]
    calls[-1:] = [calls[-1][:1], calls[-1][1:]]
    n_q = len(q_pieces)
    totals, attended, out_blocks = None, [], None

    def run(call, some, state, last, fetch):
        blocks = [block_of(by, turn, lag) for lag, turn, by in call]
        pieces = [piece_of(*key) for key in call]
        full = all(0 < lag < hops for lag, _, _ in call)
        return attend(
            numbers,
            [query_blocks[r] for r in some],
            blocks,
            [q_pieces[r] for r in some],
            pieces,
            state,
            last,
            full,
            fetch,
        )

    for index, call in enumerate(calls[:-1]):
        fetch = Fetch(row_blocks, out_fetch) if index == len(calls) - 5 else NOTHING
        totals = run(call, range(n_q), totals, False, fetch)
        if fetch is not NOTHING:
            totals, out_blocks = totals[: 2 * n_q], totals[2 * n_q :]
    for r in range(n_q):
        state = [totals[r], totals[n_q + r]]
        attended += run(calls[-1], [r], state, True, NOTHING)
    total = None
    for turn, o in enumerate(attended):
        own = gather_back(o, turn)
        lefts = [own] + [over_cores(own, by) for by in others]
        parts = [range(cores)]
        if turn == kv_heads - 1:
            parts = [range(1), range(1, cores)]
        for index, some in enumerate(parts):
            last = turn == kv_heads - 1 and index == len(parts) - 1
            out = out_projection(
                numbers, [lefts[k] for k in some], out_blocks[turn], some, total, last
            )
            total = out[0]
    share, own_squares = out
    squares = [own_squares] + [over_cores(own_squares, by) for by in others]
    return finish(tokens, share, gain_out, squares)


def solution(mesh):
    placed = (
        P("seq", "head"),
        P(),
        P(None, "head"),
        P(None, "head"),
        P(None, "head"),
        P("head", None),
        P("head"),
    )
    return jax.shard_map(
        local, mesh=mesh, in_specs=placed, out_specs=P("seq", "head"), check_vma=False
    )
```

```python
import functools

import jax
import jax.numpy as jnp
from jax import lax
from jax.experimental import pallas as pl
from jax.experimental.pallas import tpu as pltpu
from jax.sharding import PartitionSpec as P


HD = 256
WINDOW = 4096

softcap_limit = 50.0
rope_base = 10000.0
norm_epsilon = 1e-06


LOG2E = 1.4426950408889634
ROW_CHUNK = 256


def rope_tables(positions, head_dim):
    midpoint = head_dim // 2
    frequency = jnp.exp(
        -jnp.log(rope_base) * (2.0 * jnp.arange(midpoint, dtype=jnp.float32) / head_dim)
    )
    angles = positions.astype(jnp.float32)[:, None] * frequency[None, :]
    return jnp.cos(angles), jnp.sin(angles)


def dot(left, right):
    return jnp.dot(left, right, preferred_element_type=jnp.float32)


VMEM = pl.BlockSpec(memory_space=pltpu.VMEM)
SMEM = pl.BlockSpec(memory_space=pltpu.SMEM)
FAR = pl.BlockSpec(memory_space=pltpu.HBM)
MIB = 1024 * 1024
GRANT = 8
SLOW = 10**11


class Fetch:
    def __init__(self, arrays, outputs):
        self.arrays = arrays
        self.outputs = outputs
        self.plan = [(k, *block) for k, (_, blocks) in enumerate(outputs) for block in blocks]

    def shapes(self):
        return [jax.ShapeDtypeStruct(shape, jnp.bfloat16) for shape, _ in self.outputs]

    def scratch(self):
        return [pltpu.SemaphoreType.DMA((len(self.plan),))] if self.plan else []

    def start(self, numbers, arrays, outputs, arrived):
        copies = []
        for k, (index, array, row, column, shape, *starts) in enumerate(self.plan):
            source = []
            for start, size in zip(starts, shape):
                first = start or 0
                if callable(first):
                    first = pl.multiple_of(first(numbers), size)
                source.append(pl.ds(first, size))
            copy = pltpu.make_async_copy(
                arrays[array].at[source[0], source[1]],
                outputs[index].at[pl.ds(row, shape[0]), pl.ds(column, shape[1])],
                arrived.at[k],
            )
            copy.start()
            copies.append(copy)
        return copies


def kernel_call(body, fetch, numbers, operands, out_shape, scratch, grant, flops, aliases=None):
    n_operands, n_arrays = len(operands), len(fetch.arrays)
    n_out, n_fetched = len(out_shape), len(fetch.outputs)

    def kernel(numbers_ref, *refs):
        refs = list(refs)
        inputs, refs = refs[:n_operands], refs[n_operands:]
        arrays, refs = refs[:n_arrays], refs[n_arrays:]
        outputs, refs = refs[:n_out], refs[n_out:]
        fetched, refs = refs[:n_fetched], refs[n_fetched:]
        copies = []
        if fetch.plan:
            copies = fetch.start(numbers_ref, arrays, fetched, refs[-1])
            refs = refs[:-1]
        body(numbers_ref, inputs, outputs, refs)
        for copy in copies:
            copy.wait()

    moved = sum(x.size * x.dtype.itemsize for x in (*operands, *out_shape))
    return pl.pallas_call(
        kernel,
        out_shape=list(out_shape) + fetch.shapes(),
        in_specs=[SMEM] + [VMEM] * n_operands + [FAR] * n_arrays,
        out_specs=[VMEM] * (n_out + n_fetched),
        scratch_shapes=list(scratch) + fetch.scratch(),
        input_output_aliases={1 + i: o for i, o in (aliases or {}).items()},
        compiler_params=pltpu.CompilerParams(vmem_limit_bytes=grant * MIB),
        cost_estimate=pl.CostEstimate(flops=flops, bytes_accessed=moved, transcendentals=0),
    )(numbers, *operands, *fetch.arrays)


NOTHING = Fetch([], [])


def lane_sums(value, lanes):
    part = value[:, :lanes]
    for k in range(lanes, value.shape[1], lanes):
        part = part + value[:, k : k + lanes]
    return part


def sum_squares(numbers, tokens, ready, fetch):
    rows, part = tokens.shape
    lanes = min(128, part)

    def body(scalars, inputs, outputs, scratch):
        step = min(16, rows)

        def some_rows(t, carry):
            at = pl.ds(pl.multiple_of(t * step, step), step)
            total = None
            for k in range(0, part, lanes):
                value = inputs[0][at, k : k + lanes].astype(jnp.float32)
                value = value * value
                total = value if total is None else total + value
            outputs[0][at, :] = total
            return carry

        lax.fori_loop(0, rows // step, some_rows, 0, unroll=2)

    out = [jax.ShapeDtypeStruct((rows, lanes), jnp.float32)]
    return kernel_call(body, fetch, numbers, [tokens, *ready], out, [], 6, SLOW)


def write_blocks(numbers, normed, firsts, weight_refs, blocks, tables, out_ref):
    cosine, sine_part = tables
    column = 0
    for weight, width, first, turned in blocks:
        here = pl.ds(pl.multiple_of(first(numbers), width), width)
        product = None
        part = normed.shape[1] // len(firsts)
        for k, start in enumerate(firsts):
            deep = pl.ds(pl.multiple_of(start(numbers), part), part)
            term = dot(normed[:, k * part : (k + 1) * part], weight_refs[weight][deep, here])
            product = term if product is None else product + term
        for head in range(0, width, HD):
            middle, end = head + HD // 2, head + HD
            leading, trailing = product[:, head:middle], product[:, middle:end]
            if turned:
                cos, sin = cosine[...], sine_part[...]
                leading, trailing = leading * cos - trailing * sin, trailing * cos + leading * sin
            out_ref[:, column + head : column + middle] = leading.astype(jnp.bfloat16)
            out_ref[:, column + middle : column + end] = trailing.astype(jnp.bfloat16)
        column += width


def normed_projection(
    numbers, shards, firsts, gain, squares, tables, weights, blocks, fetch
):
    n = len(shards)
    rows, part = shards[0].shape

    def body(scalars, inputs, outputs, scratch):
        shard_refs, square_refs = inputs[:n], inputs[n : 2 * n]
        gain_ref, cosine, sine_part = inputs[2 * n : 2 * n + 3]
        weight_refs = inputs[2 * n + 3 :]
        normed, out_ref = outputs
        scale_ref = scratch[0]
        total = square_refs[0][...]
        for ref in square_refs[1:]:
            total = total + ref[...]
        total = jnp.sum(total, axis=-1, keepdims=True)
        scale = lax.rsqrt(total / (part * n) + norm_epsilon)
        scale_ref[...] = jnp.broadcast_to(scale, scale_ref.shape)
        gains = scratch[1]
        step = gains.shape[0]
        lanes = scale_ref.shape[1]
        for k in range(n):
            first = firsts[k](scalars)
            for column in range(0, part, lanes):
                gain = gain_ref[pl.ds((first + column) // lanes, 1), :]
                here = slice(k * part + column, k * part + column + lanes)
                gains[:, here] = jnp.broadcast_to(gain, (step, lanes))

        def norm_rows(t, carry):
            at = pl.ds(pl.multiple_of(t * step, step), step)
            scale = scale_ref[at, :]
            for k, shard in enumerate(shard_refs):
                for column in range(0, part, lanes):
                    here = slice(k * part + column, k * part + column + lanes)
                    value = shard[at, column : column + lanes].astype(jnp.float32)
                    value = value * scale * gains[:, here]
                    normed[at, here] = value.astype(jnp.bfloat16)
            return carry

        lax.fori_loop(0, rows // step, norm_rows, 0, unroll=2)
        write_blocks(scalars, normed, firsts, weight_refs, blocks, (cosine, sine_part), out_ref)

    width = sum(width for _, width, _, _ in blocks)
    out = [
        jax.ShapeDtypeStruct((rows, part * n), jnp.bfloat16),
        jax.ShapeDtypeStruct((rows, width), jnp.bfloat16),
    ]
    operands = [*shards, *squares, gain, *tables, *weights]
    flops = 2 * rows * part * n * width
    scratch = [
        pltpu.VMEM((rows, min(128, part)), jnp.float32),
        pltpu.VMEM((min(16, rows), part * n), jnp.float32),
    ]
    return kernel_call(body, fetch, numbers, operands, out, scratch, GRANT, flops)


def projection(numbers, normed, firsts, tables, weights, outputs, fetch):
    rows = normed.shape[0]

    def body(scalars, inputs, outs, scratch):
        for blocks, out_ref in zip(outputs, outs):
            write_blocks(
                scalars, inputs[0], firsts, inputs[3:], blocks, inputs[1:3], out_ref
            )

    widths = [sum(width for _, width, _, _ in blocks) for blocks in outputs]
    out = [jax.ShapeDtypeStruct((rows, width), jnp.bfloat16) for width in widths]
    flops = 2 * normed.size * sum(widths)
    return kernel_call(body, fetch, numbers, [normed, *tables, *weights], out, [], 8, flops)


def out_projection(numbers, lefts, weight, total, last):
    n = len(lefts)
    rows, width = lefts[0].shape
    out_width = weight.shape[1]
    lanes = min(128, out_width)
    columns = 256 if out_width % 256 == 0 else out_width

    def body(scalars, inputs, outputs, scratch):
        weight_ref = inputs[n]
        left = scratch[0]
        for k in range(n):
            left[:, k * width : (k + 1) * width] = inputs[k][...]
        for column in range(0, out_width, columns):
            here = slice(column, column + columns)
            value = dot(left[...], weight_ref[:, here])
            if total is not None:
                value = value + inputs[n + 1][:, here]
            outputs[0][:, here] = value
            if last:
                part = lane_sums(value * value, lanes)
                if column == 0:
                    outputs[1][...] = part
                else:
                    outputs[1][...] = outputs[1][...] + part

    out = [jax.ShapeDtypeStruct((rows, out_width), jnp.float32)]
    if last:
        out.append(jax.ShapeDtypeStruct((rows, lanes), jnp.float32))
    operands = [*lefts, weight] + ([] if total is None else [total])
    aliases = {} if total is None else {n + 1: 0}
    scratch = [pltpu.VMEM((rows, n * width), jnp.bfloat16)]
    flops = 2 * rows * n * width * out_width
    return kernel_call(body, NOTHING, numbers, operands, out, scratch, 8, flops, aliases)


def finish_kernel(n, pieces, tokens, share, gain, *refs):
    square_refs, out, held, scale_ref, copied = refs[:n], *refs[n:]
    rows, part = held.shape
    lanes = scale_ref.shape[1]
    total = square_refs[0][...]
    for ref in square_refs[1:]:
        total = total + ref[...]
    total = jnp.sum(total, axis=-1, keepdims=True)
    scale = lax.rsqrt(total / (part * n) + norm_epsilon)
    scale_ref[...] = jnp.broadcast_to(scale, scale_ref.shape)
    block = rows // pieces
    step = min(16, block)

    def some_rows(t, carry):
        at = pl.ds(pl.multiple_of(t * step, step), step)
        scale = scale_ref[at, :]
        for column in range(0, part, lanes):
            columns = slice(column, column + lanes)
            value = gain[column // lanes : column // lanes + 1, :] * share[at, columns] * scale
            value = tokens[at, columns].astype(jnp.float32) + value
            held[at, columns] = value.astype(jnp.bfloat16)
        return carry

    copies = []
    for k in range(pieces):
        steps = block // step
        lax.fori_loop(k * steps, (k + 1) * steps, some_rows, 0, unroll=2)
        at = slice(k * block, (k + 1) * block)
        copies.append(pltpu.make_async_copy(held.at[at, :], out.at[at, :], copied.at[k]))
        copies[-1].start()
    for copy in copies:
        copy.wait()


def finish(tokens, share, gain, squares):
    rows, part = tokens.shape
    pieces = 4 if rows % 64 == 0 else 1
    return pl.pallas_call(
        functools.partial(finish_kernel, len(squares), pieces),
        out_shape=jax.ShapeDtypeStruct((rows, part), jnp.bfloat16),
        in_specs=[VMEM] * (3 + len(squares)),
        out_specs=FAR,
        scratch_shapes=[
            pltpu.VMEM((rows, part), jnp.bfloat16),
            pltpu.VMEM((rows, min(128, part)), jnp.float32),
            pltpu.SemaphoreType.DMA((pieces,)),
        ],
        compiler_params=pltpu.CompilerParams(vmem_limit_bytes=8 * MIB),
        cost_estimate=pl.CostEstimate(
            flops=8 * rows * part, bytes_accessed=8 * rows * part, transcendentals=0
        ),
    )(tokens, share, gain, *squares)


def attend(numbers, query_blocks, key_blocks, queries, pieces, totals, last, full, fetch):
    n_q, n_kv = len(queries), len(pieces)
    rows, width = queries[0].shape
    heads = width // HD
    lanes = min(128, rows)
    window_blocks = WINDOW // rows
    first = totals is None
    shapes = [(rows, width)] * n_q + [(rows, heads * lanes)] * n_q
    chunk = min(ROW_CHUNK, rows)

    def body(scalars, inputs, outputs, scratch):
        q_refs, kv_refs = inputs[:n_q], inputs[n_q : n_q + n_kv]
        kv_all, key_numbers = scratch[:2]
        state = outputs[n_q:] if last else outputs
        acc, den = state[:n_q], state[n_q:]
        for k in range(n_kv):
            kv_all[k * rows : (k + 1) * rows, :] = kv_refs[k][...]
            key_numbers[k] = key_blocks[k](scalars)
        for ref in state:
            if first:
                ref[...] = jnp.zeros_like(ref)

        def add(r, keys_at, delta):
            for head in range(heads):
                for start in range(0, rows, chunk):
                    at = slice(start, start + chunk)
                    columns = slice(head * HD, (head + 1) * HD)
                    scores = lax.dot_general(
                        q_refs[r][at, columns],
                        kv_all[keys_at, :HD],
                        (((1,), (1,)), ((), ())),
                        preferred_element_type=jnp.float32,
                    )
                    weights = jnp.exp2(
                        jnp.tanh(scores * (HD ** (-0.5) / softcap_limit))
                        * (softcap_limit * LOG2E)
                    )
                    if delta is not None:
                        ahead = (
                            lax.broadcasted_iota(jnp.int32, weights.shape, 0)
                            - lax.broadcasted_iota(jnp.int32, weights.shape, 1)
                            + start
                        )
                        limit = jnp.where((delta > 0) & (delta < window_blocks), -rows, 0)
                        far = delta == window_blocks
                        weights = weights * jnp.where(
                            ahead >= limit,
                            jnp.where(far, 0.0, 1.0).astype(jnp.float32),
                            jnp.where(far, 1.0, 0.0).astype(jnp.float32),
                        )
                    lane_at = slice(head * lanes, (head + 1) * lanes)
                    den[r][at, lane_at] = den[r][at, lane_at] + lane_sums(weights, lanes)
                    acc[r][at, columns] = acc[r][at, columns] + dot(
                        weights.astype(jnp.bfloat16), kv_all[keys_at, HD:]
                    )

        if full:

            @pl.when(key_numbers[0] >= 0)
            def _():
                for r in range(n_q):
                    add(r, slice(0, n_kv * rows), None)

        else:

            def step(n, carry):
                key_block = key_numbers[n]
                live = key_block >= 0
                deltas = [block(scalars) - key_block for block in query_blocks]
                inside = [(delta > 0) & (delta < window_blocks) for delta in deltas]
                every = functools.reduce(jnp.logical_and, inside)
                keys_at = pl.ds(pl.multiple_of(n * rows, rows), rows)

                @pl.when(live & every)
                def _():
                    for r in range(n_q):
                        add(r, keys_at, None)

                for r in range(n_q):
                    some = (deltas[r] >= 0) & (deltas[r] <= window_blocks)

                    @pl.when(live & some & jnp.logical_not(every))
                    def _():
                        add(r, keys_at, deltas[r])

                return carry

            lax.fori_loop(0, n_kv, step, 0)
        if last:
            for r in range(n_q):
                for head in range(heads):
                    total = jnp.sum(
                        den[r][:, head * lanes : (head + 1) * lanes], axis=-1, keepdims=True
                    )
                    columns = slice(head * HD, (head + 1) * HD)
                    outputs[r][:, columns] = (acc[r][:, columns] / total).astype(jnp.bfloat16)

    scratch = [
        pltpu.VMEM((n_kv * rows, pieces[0].shape[1]), jnp.bfloat16),
        pltpu.SMEM((n_kv,), jnp.int32),
    ]
    operands = [*queries, *pieces] + ([] if first else list(totals))
    aliases = {}
    out = [jax.ShapeDtypeStruct(shape, jnp.float32) for shape in shapes]
    n_attended = n_q if last else 0
    out = [jax.ShapeDtypeStruct((rows, width), jnp.bfloat16)] * n_attended + out
    if not first:
        aliases = {n_q + n_kv + k: n_attended + k for k in range(2 * n_q)}
    flops = n_q * n_kv * heads * 4 * rows * rows * HD * 2 // 3
    return kernel_call(body, fetch, numbers, operands, out, scratch, 14, flops, aliases)


def local(tokens, pre_gain, query_weight, key_weight, value_weight, out_weight, post_gain):
    n_seq = lax.axis_size("seq")
    cores = lax.axis_size("head")
    rows, part = tokens.shape
    kv_heads = key_weight.shape[1] // HD
    query_heads = query_weight.shape[1] // HD
    piece_width = query_heads // kv_heads * HD
    plane = cores * kv_heads
    hops = WINDOW // (rows * plane)
    seq = lax.axis_index("seq")
    core = lax.axis_index("head")
    place = seq % plane
    column = place % kv_heads
    row = place // kv_heads

    def over_cores(value, by=1):
        return lax.ppermute(value, "head", [(c, (c + by) % cores) for c in range(cores)])

    def next_plane(value):
        return lax.ppermute(value, "seq", [(i, i + plane) for i in range(n_seq - plane)])

    def route(turn):
        pairs = []
        for s in range(n_seq):
            base, at = s - s % plane, s % plane
            y, x = at // kv_heads, at % kv_heads
            for c in range(cores):
                target = base + c * kv_heads + (x + c + turn) % kv_heads
                pairs.append((s * cores + c, target * cores + y))
        return pairs

    def spread(value, turn):
        return lax.ppermute(value, ("seq", "head"), route(turn))

    def gather_back(value, turn):
        return lax.ppermute(value, ("seq", "head"), [(b, a) for a, b in route(turn)])

    turns = range(kv_heads)
    others = range(1, cores)
    numbers = jnp.stack([core, column, row, seq - place]).astype(jnp.int32)

    def held_by(by, turn, scale):
        def start(ref):
            return lax.rem(ref[1] + lax.rem(ref[0] + cores - by, cores) + turn, kv_heads) * scale

        return start

    shards = [tokens] + [over_cores(tokens, by) for by in others]
    firsts = [
        (lambda ref, by=by: lax.rem(ref[0] + cores - by, cores) * part) for by in range(cores)
    ]
    positions = seq * rows + jnp.arange(rows, dtype=jnp.int32)
    tables = rope_tables(positions, HD)
    lanes = min(128, part)
    gain_in, gain_out = pre_gain.reshape(-1, lanes), post_gain.reshape(-1, lanes)
    (own_squares,) = sum_squares(numbers, tokens, [*tables], NOTHING)
    kv_weights = [key_weight, value_weight]
    squares = [own_squares] + [over_cores(own_squares, by) for by in others]
    kv_blocks = [
        [(n, HD, held_by(0, turn, HD), n == 0) for n in range(len(kv_weights))] for turn in turns
    ]
    q_blocks = [[(0, piece_width, held_by(0, turn, piece_width), True)] for turn in turns]
    normed, piece = normed_projection(
        numbers,
        shards,
        firsts,
        gain_in,
        squares,
        tables,
        kv_weights,
        kv_blocks[0],
        NOTHING,
    )
    sent = [piece]
    row_blocks = [out_weight]
    out_rows = out_weight.shape[0]
    for turn in turns[1:]:
        fetch = NOTHING
        if turn == 1:
            shape = (out_rows, part)
            columns = [
                (lambda ref, by=by: lax.rem(ref[0] + by, cores) * part) for by in others
            ]
            fetch = Fetch(
                [out_weight], [(shape, [(0, 0, 0, shape, None, first)]) for first in columns]
            )
        piece, *blocks = projection(
            numbers, normed, firsts, tables, kv_weights, [kv_blocks[turn]], fetch
        )
        sent.append(piece)
        row_blocks += [over_cores(block, by) for by, block in zip(others, blocks)]
    q_out = []
    for turn in turns:
        q_out += projection(
            numbers, normed, firsts, tables, [query_weight], [q_blocks[turn]], NOTHING
        )

    travelling = [next_plane(piece) for piece in sent]
    q_pieces = [spread(piece, turn) for turn, piece in enumerate(q_out)]
    levels = [[spread(piece, turn) for turn, piece in enumerate(sent)]]
    level = [spread(piece, turn) for turn, piece in enumerate(travelling)]
    levels.append(level)
    for _ in range(2, hops + 1):
        level = [next_plane(piece) for piece in level]
        levels.append(level)

    def block_of(by, turn, lag):
        def block(ref):
            column_of = lax.rem(ref[1] - ref[2] - turn + cores * plane * kv_heads, kv_heads)
            row_of = lax.rem(ref[0] + cores - by, cores)
            return ref[3] - lag * plane + row_of * kv_heads + column_of

        return block

    query_blocks = [block_of(0, turn, 0) for turn in turns]

    merged = {}

    def piece_of(lag, turn, by):
        if (lag, turn, by) not in merged:
            piece = levels[lag][turn]
            merged[lag, turn, by] = over_cores(piece, by) if by else piece
        return merged[lag, turn, by]

    out_fetch = []
    for by in range(cores):
        blocks = []
        for turn in turns:
            blocks.append(
                (
                    by,
                    turn * piece_width,
                    0,
                    (piece_width, part),
                    held_by(by, turn, piece_width),
                    None if by else (lambda ref: ref[0] * part),
                )
            )
        out_fetch.append(((piece_width * kv_heads, part), blocks))
    calls = [[(0, 0, by) for by in range(cores)]]
    for lag in range(1, hops + 1):
        for turn in turns:
            calls.append([(lag, turn, by) for by in range(cores)])
    calls[-1:-1] = [[(0, turn, by) for by in range(cores)] for turn in turns[1:]]
    n_q = len(q_pieces)
    totals, attended, out_blocks = None, [], None

    def run(call, some, state, last, fetch):
        blocks = [block_of(by, turn, lag) for lag, turn, by in call]
        pieces = [piece_of(*key) for key in call]
        full = all(0 < lag < hops for lag, _, _ in call)
        return attend(
            numbers,
            [query_blocks[r] for r in some],
            blocks,
            [q_pieces[r] for r in some],
            pieces,
            state,
            last,
            full,
            fetch,
        )

    for index, call in enumerate(calls[:-1]):
        fetch = Fetch(row_blocks, out_fetch) if index == len(calls) - 4 else NOTHING
        totals = run(call, range(n_q), totals, False, fetch)
        if fetch is not NOTHING:
            totals, out_blocks = totals[: 2 * n_q], totals[2 * n_q :]
    for r in range(n_q):
        state = [totals[r], totals[n_q + r]]
        call = calls[-1]
        if r == 0:
            state = run(call[:1], [r], state, False, NOTHING)
            call = call[1:]
        attended += run(call, [r], state, True, NOTHING)[:1]
    total = None
    back = [gather_back(o, turn) for turn, o in enumerate(attended)]
    for by in range(cores):
        lefts = back
        if by:
            lefts = [over_cores(own, by) for own in back]
        out = out_projection(numbers, lefts, out_blocks[by], total, by == cores - 1)
        total = out[0]
    share, own_squares = out
    squares = [own_squares] + [over_cores(own_squares, by) for by in others]
    return finish(tokens, share, gain_out, squares)


def solution(mesh):
    placed = (
        P("seq", "head"),
        P(),
        P(None, "head"),
        P(None, "head"),
        P(None, "head"),
        P("head", None),
        P("head"),
    )
    return jax.shard_map(
        local, mesh=mesh, in_specs=placed, out_specs=P("seq", "head"), check_vma=False
    )
```
